128 devices in a mesh: outer: 8 (over z_hi, y), inner: 16 (over z_lo, x, core).
Axes of the slice: x: 4, y: 4, z: 4 (z_hi: 2, z_lo: 2; z = z_hi * 2 + z_lo), core: 2. Of those that a mesh axis runs over, the one named last changes fastest.
Arguments:
- query_rows: bfloat16 [16384, 4096], P(('outer', 'inner')), may hold values from -6 to 6
- key_rows: bfloat16 [16384, 4096], P(('outer', 'inner')), may hold values from -6 to 6
- value_rows: bfloat16 [16384, 4096], P(('outer', 'inner')), may hold values from -6 to 6
- out_grad: bfloat16 [16384, 4096], P(('outer', 'inner')), may hold values from -6 to 6
- filter_rows: bfloat16 [16384, 4096], P(('outer', 'inner')), may hold values from -0.046875 to 0.046875
- skip_gain: float32 [4096], replicated, may hold values from -1 to 1
Outputs:
- layer_out: bfloat16 [16384, 4096], P(('outer', 'inner'))
- query_grad: bfloat16 [16384, 4096], P(('outer', 'inner'))
- key_grad: bfloat16 [16384, 4096], P(('outer', 'inner'))
- value_grad: bfloat16 [16384, 4096], P(('outer', 'inner'))
- filter_grad: bfloat16 [16384, 4096], P(('outer', 'inner'))
- skip_grad: float32 [4096], replicated
The draws below stay inside these ranges and needn't reach their ends.
All inputs are finite; a program needn't handle non-finite values.
Results may differ from the reference program's by a relative error of at most 0.0085.
Values may be sent and summed in bfloat16 or wider, within the bound.
A program may use at most 128 MiB of HBM per device.

```python
import math
import jax
import jax.numpy as jnp
from jax import lax

CHANNELS = 4096
TOK_DEV = 128
TOKENS = 16384
N_OUTER = 8
N_INNER = 16


def steps_of(rng, shape, cuts, smallest, largest):
    def one(dim, blocks):
        heights = jax.random.uniform(jax.random.fold_in(jax.random.fold_in(rng, 6), dim), (blocks,), jnp.float32, smallest / len(cuts), largest / len(cuts))
        return jnp.repeat(jnp.exp(heights), shape[dim] // blocks).reshape((-1,) + (1,) * (len(shape) - dim - 1))

    loudness = one(*cuts[0])
    for cut in cuts[1:]:
        loudness = loudness * one(*cut)
    return loudness


def noise(stream_key, dims, scale, limit, shards=(), held_as=jnp.bfloat16):
    factor_of = steps_of(stream_key, dims, shards, -0.22, 0.18) if shards else 1.0
    values = jax.random.normal(stream_key, dims, jnp.float32) * scale * factor_of
    return jnp.minimum(jnp.maximum(values, -limit), limit).astype(held_as)


def setup_inputs(seed: int = 0) -> dict:
    keys = jax.random.split(jax.random.key(seed), 7)
    return {
        "query_rows": noise(keys[0], (TOKENS, CHANNELS), 1.0, 6.0, ((0, 128),)),
        "key_rows": noise(keys[1], (TOKENS, CHANNELS), 1.0, 6.0, ((0, 128),)),
        "value_rows": noise(keys[2], (TOKENS, CHANNELS), 1.0, 6.0, ((0, 128),)),
        "out_grad": noise(keys[3], (TOKENS, CHANNELS), 1.0, 6.0, ((0, 128),)),
        "filter_rows": noise(keys[4], (TOKENS, CHANNELS), TOKENS ** -0.5, 0.046875, ((0, 128),)),
        "skip_gain": jnp.clip(jax.random.uniform(keys[5], (CHANNELS,), jnp.float32, -1.0, 1.0), -1.0, 1.0),
    }


TWO_PI = 2.0 * math.pi
HIGH = lax.Precision.HIGHEST

def settle(values):
    rounded = values.astype(jnp.bfloat16)
    return lax.optimization_barrier(rounded).astype(jnp.float32)

def rounded_trig(phase, modulus):
    angle = (phase % modulus).astype(jnp.float32) * (TWO_PI / modulus)
    return (settle(jnp.cos(angle)), settle(jnp.sin(angle)))

def make_tables():
    devices = N_OUTER * N_INNER
    radix_count = 2 * devices
    points = 2 * TOKENS
    rows = jnp.arange(devices, dtype=jnp.int32)
    freqs = jnp.arange(radix_count, dtype=jnp.int32)
    steps = jnp.arange(TOK_DEV, dtype=jnp.int32)
    first_phase = rows[None, None, :] * freqs[None, :, None] * TOK_DEV + steps[:, None, None] * freqs[None, :, None]
    first = rounded_trig(first_phase, points)
    second = rounded_trig(steps[:, None] * steps[None, :], TOK_DEV)
    third_phase = steps[None, :, None] * steps[None, None, :] * radix_count + steps[None, :, None] * freqs[:, None, None]
    third = rounded_trig(third_phase, points)
    last = rounded_trig(rows[:, None] * freqs[None, :], radix_count)
    return (first, second, third, last)

def spectrum_of(signal, tables):
    devices = N_OUTER * N_INNER
    (first_cos, first_sin), (step_cos, step_sin) = (tables[0], tables[1])
    width = signal.shape[1]
    grid = signal.astype(jnp.float32).reshape(devices, TOK_DEV, width)
    one_real = settle(jnp.einsum('skr,rsc->ksc', first_cos, grid, precision=HIGH))
    one_imag = settle(-jnp.einsum('skr,rsc->ksc', first_sin, grid, precision=HIGH))
    spec_real = jnp.einsum('ksc,sq->kqc', one_real, step_cos, precision=HIGH) + jnp.einsum('ksc,sq->kqc', one_imag, step_sin, precision=HIGH)
    spec_imag = jnp.einsum('ksc,sq->kqc', one_imag, step_cos, precision=HIGH) - jnp.einsum('ksc,sq->kqc', one_real, step_sin, precision=HIGH)
    return (spec_real, spec_imag)

def inverse_of(q_real, q_imag, tables):
    devices = N_OUTER * N_INNER
    points = 2 * TOKENS
    (third_cos, third_sin), (last_cos, last_sin) = (tables[2], tables[3])
    q_real = settle(q_real)
    q_imag = settle(q_imag)
    three_real = settle(jnp.einsum('kqc,ksq->ksc', q_real, third_cos, precision=HIGH) - jnp.einsum('kqc,ksq->ksc', q_imag, third_sin, precision=HIGH))
    three_imag = settle(jnp.einsum('kqc,ksq->ksc', q_real, third_sin, precision=HIGH) + jnp.einsum('kqc,ksq->ksc', q_imag, third_cos, precision=HIGH))
    values = (jnp.einsum('rk,ksc->rsc', last_cos, three_real, precision=HIGH) - jnp.einsum('rk,ksc->rsc', last_sin, three_imag, precision=HIGH)) / points
    return values.reshape(devices * TOK_DEV, values.shape[2]).astype(jnp.bfloat16)

def reference(query_rows, key_rows, value_rows, out_grad, filter_rows, skip_gain):
    factor = 1.0 / math.sqrt(TOKENS)
    product = (key_rows.astype(jnp.float32) * value_rows.astype(jnp.float32)).astype(jnp.bfloat16)
    gate_grad = out_grad.astype(jnp.float32) * query_rows.astype(jnp.float32)
    gate_half = gate_grad.astype(jnp.bfloat16)
    tables = make_tables()
    block = math.gcd(CHANNELS, 256)
    count = CHANNELS // block

    def per_block(index):
        start = (index * block).astype(jnp.int32)
        product_block = lax.dynamic_slice_in_dim(product, start, block, 1)
        gate_block = lax.dynamic_slice_in_dim(gate_half, start, block, 1)
        filter_block = lax.dynamic_slice_in_dim(filter_rows, start, block, 1)
        value_real, value_imag = spectrum_of(product_block, tables)
        gate_real, gate_imag = spectrum_of(gate_block, tables)
        filter_real, filter_imag = spectrum_of(filter_block, tables)
        convolved = inverse_of(value_real * filter_real - value_imag * filter_imag, value_real * filter_imag + value_imag * filter_real, tables)
        correlated = inverse_of(filter_real * gate_real + filter_imag * gate_imag, filter_real * gate_imag - filter_imag * gate_real, tables)
        lagged = inverse_of((value_real * gate_real + value_imag * gate_imag) * factor, (value_real * gate_imag - value_imag * gate_real) * factor, tables)
        return (convolved, correlated, lagged)
    convolved, correlated, lagged = lax.map(per_block, jnp.arange(count, dtype=jnp.int32))
    convolved = convolved.transpose(1, 0, 2).reshape(TOKENS, CHANNELS).astype(jnp.float32)
    correlated = correlated.transpose(1, 0, 2).reshape(TOKENS, CHANNELS).astype(jnp.float32)
    filter_grad = lagged.transpose(1, 0, 2).reshape(TOKENS, CHANNELS)
    product_full = product.astype(jnp.float32)
    mixing = convolved + skip_gain[None, :] * product_full
    layer_out = (query_rows.astype(jnp.float32) * mixing).astype(jnp.bfloat16)
    query_grad = (out_grad.astype(jnp.float32) * mixing).astype(jnp.bfloat16)
    carried = correlated + skip_gain[None, :] * gate_grad
    key_grad = (carried * value_rows.astype(jnp.float32)).astype(jnp.bfloat16)
    value_grad = (carried * key_rows.astype(jnp.float32)).astype(jnp.bfloat16)
    skip_grad = lax.optimization_barrier(jnp.sum(gate_grad * product_full, axis=0)) * factor
    return (layer_out, query_grad, key_grad, value_grad, filter_grad, skip_grad)
```

```python
import functools
import math

import jax
import jax.numpy as jnp
import numpy as np
from jax import lax
from jax.experimental import pallas as pl
from jax.experimental.pallas import tpu as pltpu
from jax.sharding import PartitionSpec as P

MESH = pl.DeviceIdType.MESH
BF = jnp.bfloat16
F32 = jnp.float32
DEVICES = 128
GROUPS = 4
ORDER = 91


def coefficient_tables(tokens, devices, length):
    pos = np.arange(devices, dtype=np.float64)
    freq = np.arange(devices, dtype=np.float64) + 0.5
    step = np.arange(tokens, dtype=np.float64)
    one = 2.0 * np.pi * np.outer(freq, pos) / (2 * devices)
    first = np.zeros((2, 2, devices, devices, 2))
    for e in range(2):
        first[e, 0, :, :, e] = np.cos(one)
        first[e, 1, :, :, e] = -np.sin(one)
    first = first.reshape(4 * devices, 2 * devices)
    last = np.transpose(first) * (2.0 / (2 * length))
    two = 2.0 * np.pi * (np.outer(step, step) % tokens) / tokens
    c, s = np.cos(two), np.sin(two)
    forth = np.block([[c, -s], [s, c]])
    back = np.block([[c, s], [-s, c]])
    turn = 2.0 * np.pi * np.outer(freq, step) / (2 * length)
    as_bf = lambda t: np.asarray(t, np.float32).astype(jnp.bfloat16)
    return (
        as_bf(first),
        as_bf(forth),
        as_bf(back),
        as_bf(last),
        np.stack([np.cos(turn), np.sin(turn)]).astype(np.float32),
    )


def kernel(
    q_hbm,
    k_hbm,
    v_hbm,
    g_hbm,
    h_hbm,
    gain_ref,
    t1_ref,
    t2_ref,
    t3_ref,
    t4_ref,
    tw_ref,
    lo_hbm,
    qg_hbm,
    kg_hbm,
    vg_hbm,
    fg_hbm,
    sk_ref,
    ins,
    outs,
    packed,
    held,
    made,
    back,
    part,
    spec,
    sk_own,
    sk_all,
    load_sem,
    store_sem,
    in_send,
    in_recv,
    out_send,
    out_recv,
    sk_send,
    sk_recv,
):
    tokens, channels = q_hbm.shape
    width = channels // GROUPS
    per = width // DEVICES
    pairs = per // 2
    outer = lax.axis_index("outer")
    inner = lax.axis_index("inner")
    me = outer * 16 + inner
    my_y, my_zh = lax.rem(outer, 4), lax.div(outer, 4)
    my_c, my_x, my_zl = lax.rem(inner, 2), lax.rem(lax.div(inner, 2), 4), lax.div(inner, 8)
    my_z = my_zh * 2 + my_zl

    def target(k):
        j = lax.rem(k * ORDER, DEVICES)
        c = lax.rem(my_c + j, 2)
        x = lax.rem(my_x + lax.div(j, 2), 4)
        y = lax.rem(my_y + lax.div(j, 8), 4)
        z = lax.rem(my_z + lax.div(j, 32), 4)
        return lax.div(z, 2) * 4 + y, lax.rem(z, 2) * 8 + x * 2 + c

    barrier = pltpu.get_barrier_semaphore()

    def greet(k, carry):
        pl.semaphore_signal(barrier, inc=1, device_id=target(k), device_id_type=MESH)
        return carry

    hbm_in = (k_hbm, v_hbm, g_hbm, q_hbm, h_hbm)
    K, V, G, Q, H = range(5)

    def load(n, g):
        cols = pl.ds(pl.multiple_of(g * width, width), width)
        return pltpu.make_async_copy(hbm_in[n].at[:, cols], ins.at[n, :, cols], load_sem.at[n, g])

    for g in range(GROUPS):
        for n in range(5):
            load(n, g).start()
    lax.fori_loop(1, DEVICES, greet, 0)

    def block_cols(g, b):
        return pl.ds(pl.multiple_of(g * width + b * 128, 128), 128)

    def prepare(g):
        for n in range(5):
            load(n, g).wait()

        def block(b, carry):
            cols = block_cols(g, b)
            rows = pl.ds(pl.multiple_of(b * 128, 128), 128)
            product = ins[K, :, cols].astype(F32) * ins[V, :, cols].astype(F32)
            gate = ins[G, :, cols].astype(F32) * ins[Q, :, cols].astype(F32)
            packed.reshape(GROUPS, 3, width, 128)[g, 0, rows, :] = product.astype(BF).T
            packed.reshape(GROUPS, 3, width, 128)[g, 1, rows, :] = gate.astype(BF).T
            packed.reshape(GROUPS, 3, width, 128)[g, 2, rows, :] = ins[H, :, cols].T
            return carry

        lax.fori_loop(0, width // 128, block, 0)

    def send_in(g):
        def one(k, carry):
            o, i = target(k)
            pltpu.make_async_remote_copy(
                src_ref=packed.at[g, :, pl.ds((o * 16 + i) * pairs, pairs)],
                dst_ref=held.at[g, :, :, pl.ds(me * 2, 2), :],
                send_sem=in_send,
                recv_sem=in_recv.at[g],
                device_id=(o, i),
                device_id_type=MESH,
            ).start()
            return carry

        pltpu.make_async_copy(
            packed.at[g, :, pl.ds(me * pairs, pairs)],
            held.at[g, :, :, pl.ds(me * 2, 2), :],
            in_recv.at[g],
        ).start()
        lax.fori_loop(1, DEVICES, one, 0)

    def send_out(g):
        def one(k, carry):
            o, i = target(k)
            pltpu.make_async_remote_copy(
                src_ref=made.at[g, :, :, pl.ds((o * 16 + i) * 2, 2), :],
                dst_ref=back.at[g, :, pl.ds(me * pairs, pairs)],
                send_sem=out_send,
                recv_sem=out_recv.at[g],
                device_id=(o, i),
                device_id_type=MESH,
            ).start()
            return carry

        pltpu.make_async_copy(
            made.at[g, :, :, pl.ds(me * 2, 2), :],
            back.at[g, :, pl.ds(me * pairs, pairs)],
            out_recv.at[g],
        ).start()
        lax.fori_loop(1, DEVICES, one, 0)

    def transform(g, h):
        wr, wi = tw_ref[0], tw_ref[1]
        pair = h * 2
        for n in range(3):
            rhs = jnp.concatenate([held[g, n, pair], held[g, n, pair + 1]], axis=1)
            one = jnp.dot(t1_ref[...], rhs, preferred_element_type=F32)
            for e in range(2):
                for p in range(2):
                    re = one[e * 256 : e * 256 + 128, p * 128 : p * 128 + 128]
                    im = one[e * 256 + 128 : e * 256 + 256, p * 128 : p * 128 + 128]
                    ch = p * 2 + e
                    part[n, ch, :, 0:128] = (re * wr + im * wi).astype(BF)
                    part[n, ch, :, 128:256] = (im * wr - re * wi).astype(BF)
        for ch in range(4):
            sp = []
            for n in range(3):
                sp.append(jnp.dot(part[n, ch], t2_ref[...], preferred_element_type=F32))
            vr, vi = sp[0][:, :128], sp[0][:, 128:]
            gr, gi = sp[1][:, :128], sp[1][:, 128:]
            fr, fi = sp[2][:, :128], sp[2][:, 128:]
            prods = (
                (vr * fr - vi * fi, vr * fi + vi * fr),
                (fr * gr + fi * gi, fr * gi - fi * gr),
                (vr * gr + vi * gi, vr * gi - vi * gr),
            )
            for n in range(3):
                qq = jnp.concatenate([prods[n][0].astype(BF), prods[n][1].astype(BF)], axis=1)
                three = jnp.dot(qq, t3_ref[...], preferred_element_type=F32)
                re, im = three[:, :128], three[:, 128:]
                p, e = ch // 2, ch % 2
                spec[n, e * 256 : e * 256 + 128, p * 128 : p * 128 + 128] = (
                    re * wr - im * wi
                ).astype(BF)
                spec[n, e * 256 + 128 : e * 256 + 256, p * 128 : p * 128 + 128] = (
                    im * wr + re * wi
                ).astype(BF)
        for n in range(3):
            four = jnp.dot(t4_ref[...], spec[n], preferred_element_type=F32)
            if n == 2:
                four = four * (1.0 / 128.0)
            for p in range(2):
                made[g, n, pair + p] = four[:, p * 128 : p * 128 + 128].astype(BF)

    lane = lax.broadcasted_iota(jnp.int32, (1, 128), 1)
    sub = lax.broadcasted_iota(jnp.int32, (8, 128), 0)

    def direct_sums(g):
        row = jnp.zeros((1, 128), F32)
        for p in range(pairs):
            terms = held[g, 0, p].astype(F32) * held[g, 1, p].astype(F32)
            folded = jnp.sum(terms.reshape(32, 8, 128), axis=0)
            for e in range(2):
                own = jnp.where(lax.rem(sub, 2) == e, folded, 0.0)
                total = jnp.sum(jnp.sum(own, axis=1, keepdims=True), axis=0, keepdims=True)
                row = row + jnp.where(lane == g * per + p * 2 + e, total, 0.0)
        sk_own[...] = sk_own[...] + row

    def send_sums():
        def one(k, carry):
            pltpu.make_async_remote_copy(
                src_ref=sk_own,
                dst_ref=sk_all.at[pl.ds(me, 1), :],
                send_sem=sk_send,
                recv_sem=sk_recv,
                device_id=target(k),
                device_id_type=MESH,
            ).start()
            return carry

        pltpu.make_async_copy(sk_own, sk_all.at[pl.ds(me, 1), :], sk_recv).start()
        lax.fori_loop(1, DEVICES, one, 0)

    def spread_sums():
        pltpu.make_async_copy(sk_all, sk_all, sk_recv).wait()
        rows = lax.broadcasted_iota(jnp.int32, (128, 128), 0)
        cols = lax.broadcasted_iota(jnp.int32, (128, 128), 1)
        mine = lax.div(cols, per) == lax.rem(rows, 16)
        for g in range(GROUPS):
            pick = (rows == g * per + lax.rem(cols, per)).astype(F32)
            wide = jnp.dot(
                sk_all[...], pick, preferred_element_type=F32, precision=lax.Precision.HIGHEST
            )
            kept = jnp.where(mine, wide, 0.0)
            sk_ref[g * 8 : g * 8 + 8, :] = jnp.sum(kept.reshape(8, 16, 128), axis=1) * (
                1.0 / 128.0
            )

    hbm_out = (lo_hbm, qg_hbm, kg_hbm, vg_hbm, fg_hbm)

    def store(n, g):
        cols = pl.ds(pl.multiple_of(g * width, width), width)
        return pltpu.make_async_copy(outs.at[n, :, cols], hbm_out[n].at[:, cols], store_sem.at[n, g])

    def finish(g):
        pltpu.make_async_copy(back.at[g], back.at[g], out_recv.at[g]).wait()

        def block(b, carry):
            cols = block_cols(g, b)
            rows = pl.ds(pl.multiple_of(b * 128, 128), 128)
            views = back.reshape(GROUPS, 3, width, 128)
            conv = views[g, 0, rows, :].T.astype(F32)
            corr = views[g, 1, rows, :].T.astype(F32)
            gain = gain_ref[pl.ds(g * (width // 128) + b, 1), :]
            kk, vv = ins[K, :, cols].astype(F32), ins[V, :, cols].astype(F32)
            gg, qq = ins[G, :, cols].astype(F32), ins[Q, :, cols].astype(F32)
            product = (kk * vv).astype(BF).astype(F32)
            mixing = conv + gain * product
            outs[0, :, cols] = (qq * mixing).astype(BF)
            outs[1, :, cols] = (gg * mixing).astype(BF)
            carried = corr + gain * (gg * qq)
            outs[2, :, cols] = (carried * vv).astype(BF)
            outs[3, :, cols] = (carried * kk).astype(BF)
            outs[4, :, cols] = views[g, 2, rows, :].T
            return carry

        lax.fori_loop(0, width // 128, block, 0)
        for n in range(5):
            store(n, g).start()

    sk_own[...] = jnp.zeros_like(sk_own)
    prepare(0)
    pl.semaphore_wait(barrier, DEVICES - 1)
    send_in(0)

    def ahead(g, carry):
        prepare(g)
        send_in(g)
        return carry

    lax.fori_loop(1, GROUPS, ahead, 0)

    def middle(g, carry):
        pltpu.make_async_copy(held.at[g], held.at[g], in_recv.at[g]).wait()

        def half(h, inside):
            transform(g, h)
            return inside

        lax.fori_loop(0, pairs // 2, half, 0)
        send_out(g)
        direct_sums(g)
        return carry

    lax.fori_loop(0, GROUPS, middle, 0)
    send_sums()

    def ending(g, carry):
        finish(g)
        return carry

    lax.fori_loop(0, GROUPS, ending, 0)
    spread_sums()
    everyone = held.at[:, :, :, pl.ds(0, 2 * (DEVICES - 1)), :]
    pltpu.make_async_copy(everyone, everyone, in_send).wait()
    pltpu.make_async_copy(everyone, everyone, out_send).wait()
    sums = sk_all.at[pl.ds(0, DEVICES - 1), :]
    pltpu.make_async_copy(sums, sums, sk_send).wait()
    for g in range(GROUPS):
        for n in range(5):
            store(n, g).wait()


def body(query_rows, key_rows, value_rows, out_grad, filter_rows, skip_gain):
    tokens, channels = query_rows.shape
    length = tokens * DEVICES
    width = channels // GROUPS
    per = width // DEVICES
    tables = [jnp.asarray(t) for t in coefficient_tables(tokens, DEVICES, length)]
    rows = jax.ShapeDtypeStruct((tokens, channels), BF)
    anywhere = pl.BlockSpec(memory_space=pl.ANY)
    vmem = pl.BlockSpec(memory_space=pltpu.VMEM)
    dma = pltpu.SemaphoreType.DMA
    results = pl.pallas_call(
        kernel,
        out_shape=[rows] * 5 + [jax.ShapeDtypeStruct((channels // 128, 128), F32)],
        in_specs=[anywhere] * 5 + [vmem] * 6,
        out_specs=[anywhere] * 5 + [vmem],
        scratch_shapes=[
            pltpu.VMEM((5, tokens, channels), BF),
            pltpu.VMEM((5, tokens, channels), BF),
            pltpu.VMEM((GROUPS, 3, width // 2, 2, 128), BF),
            pltpu.VMEM((GROUPS, 3, per // 2, 2 * DEVICES, 128), BF),
            pltpu.VMEM((GROUPS, 3, per // 2, 2 * DEVICES, 128), BF),
            pltpu.VMEM((GROUPS, 3, width // 2, 2, 128), BF),
            pltpu.VMEM((3, 4, DEVICES, 256), BF),
            pltpu.VMEM((3, 4 * DEVICES, 256), BF),
            pltpu.VMEM((1, 128), F32),
            pltpu.VMEM((DEVICES, 128), F32),
            dma((5, GROUPS)),
            dma((5, GROUPS)),
            dma,
            dma((GROUPS,)),
            dma,
            dma((GROUPS,)),
            dma,
            dma,
        ],
        compiler_params=pltpu.CompilerParams(
            collective_id=0, has_side_effects=True, vmem_limit_bytes=56 * 1024 * 1024
        ),
        name="hyena",
    )(
        query_rows,
        key_rows,
        value_rows,
        out_grad,
        filter_rows,
        skip_gain.reshape(channels // 128, 128),
        *tables,
    )
    return (*results[:5], results[5].reshape(channels))


def solution(mesh):
    rows = P(("outer", "inner"), None)
    return jax.shard_map(
        body,
        mesh=mesh,
        in_specs=(rows, rows, rows, rows, rows, P()),
        out_specs=(rows, rows, rows, rows, rows, P()),
        check_vma=False,
    )
```

```python
import functools
import math

import jax
import jax.numpy as jnp
import numpy as np
from jax import lax
from jax.experimental import pallas as pl
from jax.experimental.pallas import tpu as pltpu
from jax.sharding import PartitionSpec as P

MESH = pl.DeviceIdType.MESH
BF = jnp.bfloat16
F32 = jnp.float32
DEVICES = 128
GROUPS = 4
ORDER = 91


def coefficient_tables(tokens, devices, length):
    pos = np.arange(devices, dtype=np.float64)
    freq = np.arange(devices, dtype=np.float64) + 0.5
    step = np.arange(tokens, dtype=np.float64)
    one = 2.0 * np.pi * np.outer(freq, pos) / (2 * devices)
    first = np.zeros((2, 2, devices, devices, 2))
    for e in range(2):
        first[e, 0, :, :, e] = np.cos(one)
        first[e, 1, :, :, e] = -np.sin(one)
    first = first.reshape(4 * devices, 2 * devices)
    last = np.transpose(first) * (2.0 / (2 * length))
    two = 2.0 * np.pi * (np.outer(step, step) % tokens) / tokens
    c, s = np.cos(two), np.sin(two)
    forth = np.block([[c, -s], [s, c]])
    back = np.block([[c, s], [-s, c]])
    turn = 2.0 * np.pi * np.outer(freq, step) / (2 * length)
    as_bf = lambda t: np.asarray(t, np.float32).astype(jnp.bfloat16)
    return (
        as_bf(first),
        as_bf(forth),
        as_bf(back),
        as_bf(last),
        np.stack([np.cos(turn), np.sin(turn)]).astype(np.float32),
    )


def kernel(
    q_hbm,
    k_hbm,
    v_hbm,
    g_hbm,
    h_hbm,
    gain_hbm,
    t1_hbm,
    t2_hbm,
    t3_hbm,
    t4_hbm,
    tw_hbm,
    lo_hbm,
    qg_hbm,
    kg_hbm,
    vg_hbm,
    fg_hbm,
    sk_hbm,
    gain_ref,
    t1_ref,
    t2_ref,
    t3_ref,
    t4_ref,
    tw_ref,
    sk_ref,
    ins,
    outs,
    packed,
    held,
    made,
    back,
    part,
    spec,
    sk_own,
    sk_all,
    load_sem,
    table_sem,
    store_sem,
    in_send,
    in_recv,
    out_send,
    out_recv,
    sk_send,
    sk_recv,
):
    tokens, channels = q_hbm.shape
    width = channels // GROUPS
    per = width // DEVICES
    pairs = per // 2
    outer = lax.axis_index("outer")
    inner = lax.axis_index("inner")
    me = outer * 16 + inner
    my_y, my_zh = lax.rem(outer, 4), lax.div(outer, 4)
    my_c, my_x, my_zl = lax.rem(inner, 2), lax.rem(lax.div(inner, 2), 4), lax.div(inner, 8)
    my_z = my_zh * 2 + my_zl

    def target(k):
        j = lax.rem(k * ORDER, DEVICES)
        c = lax.rem(my_c + j, 2)
        x = lax.rem(my_x + lax.div(j, 2), 4)
        y = lax.rem(my_y + lax.div(j, 8), 4)
        z = lax.rem(my_z + lax.div(j, 32), 4)
        return lax.div(z, 2) * 4 + y, lax.rem(z, 2) * 8 + x * 2 + c

    barrier = pltpu.get_barrier_semaphore()
    row = my_x * 2 + my_c

    def greet():
        for dz in (2, 1, 3, 0):
            z = lax.rem(my_z + dz, 4)
            for dy in (2, 1, 3, 0):
                o = lax.div(z, 2) * 4 + lax.rem(my_y + dy, 4)
                base = lax.rem(z, 2) * 8
                alone = dz == 0 and dy == 0

                def one(t, carry):
                    i = base + (lax.rem(row + t, 8) if alone else t)
                    pl.semaphore_signal(barrier, inc=1, device_id=(o, i), device_id_type=MESH)
                    return carry

                lax.fori_loop(1 if alone else 0, 8, one, 0)

    hbm_in = (k_hbm, v_hbm, g_hbm, q_hbm, h_hbm)
    K, V, G, Q, H = range(5)

    def load(n, g):
        cols = pl.ds(pl.multiple_of(g * width, width), width)
        return pltpu.make_async_copy(hbm_in[n].at[:, cols], ins.at[n, :, cols], load_sem.at[n, g])

    for n in range(5):
        load(n, 0).start()
    greet()
    for g in range(1, GROUPS):
        for n in range(5):
            load(n, g).start()
    fixed = (
        (t1_hbm, t1_ref),
        (t2_hbm, t2_ref),
        (t3_hbm, t3_ref),
        (t4_hbm, t4_ref),
        (tw_hbm, tw_ref),
        (gain_hbm, gain_ref),
    )
    for n, (source, place) in enumerate(fixed):
        pltpu.make_async_copy(source, place, table_sem.at[n]).start()

    def block_cols(g, b):
        return pl.ds(pl.multiple_of(g * width + b * 128, 128), 128)

    def prepare(g):
        for n in range(5):
            load(n, g).wait()

        def block(b, carry):
            cols = block_cols(g, b)
            rows = pl.ds(pl.multiple_of(b * 128, 128), 128)
            product = ins[K, :, cols].astype(F32) * ins[V, :, cols].astype(F32)
            gate = ins[G, :, cols].astype(F32) * ins[Q, :, cols].astype(F32)
            packed.reshape(GROUPS, 3, width, 128)[g, 0, rows, :] = product.astype(BF).T
            packed.reshape(GROUPS, 3, width, 128)[g, 1, rows, :] = gate.astype(BF).T
            packed.reshape(GROUPS, 3, width, 128)[g, 2, rows, :] = ins[H, :, cols].T
            return carry

        lax.fori_loop(0, width // 128, block, 0)

    def send_in(g):
        def one(k, carry):
            o, i = target(k)
            pltpu.make_async_remote_copy(
                src_ref=packed.at[g, :, pl.ds((o * 16 + i) * pairs, pairs)],
                dst_ref=held.at[g, :, :, pl.ds(me * 2, 2), :],
                send_sem=in_send,
                recv_sem=in_recv.at[g],
                device_id=(o, i),
                device_id_type=MESH,
            ).start()
            return carry

        pltpu.make_async_copy(
            packed.at[g, :, pl.ds(me * pairs, pairs)],
            held.at[g, :, :, pl.ds(me * 2, 2), :],
            in_recv.at[g],
        ).start()
        lax.fori_loop(1, DEVICES, one, 0)

    def send_out(g):
        def one(k, carry):
            o, i = target(k)
            pltpu.make_async_remote_copy(
                src_ref=made.at[g, :, :, pl.ds((o * 16 + i) * 2, 2), :],
                dst_ref=back.at[g, :, pl.ds(me * pairs, pairs)],
                send_sem=out_send,
                recv_sem=out_recv.at[g],
                device_id=(o, i),
                device_id_type=MESH,
            ).start()
            return carry

        pltpu.make_async_copy(
            made.at[g, :, :, pl.ds(me * 2, 2), :],
            back.at[g, :, pl.ds(me * pairs, pairs)],
            out_recv.at[g],
        ).start()
        lax.fori_loop(1, DEVICES, one, 0)

    def transform(g, h):
        wr, wi = tw_ref[0], tw_ref[1]
        pair = h * 2
        for n in range(3):
            rhs = jnp.concatenate([held[g, n, pair], held[g, n, pair + 1]], axis=1)
            one = jnp.dot(t1_ref[...], rhs, preferred_element_type=F32)
            for e in range(2):
                for p in range(2):
                    re = one[e * 256 : e * 256 + 128, p * 128 : p * 128 + 128]
                    im = one[e * 256 + 128 : e * 256 + 256, p * 128 : p * 128 + 128]
                    ch = p * 2 + e
                    part[n, ch, :, 0:128] = (re * wr + im * wi).astype(BF)
                    part[n, ch, :, 128:256] = (im * wr - re * wi).astype(BF)
        for ch in range(4):
            sp = []
            for n in range(3):
                sp.append(jnp.dot(part[n, ch], t2_ref[...], preferred_element_type=F32))
            vr, vi = sp[0][:, :128], sp[0][:, 128:]
            gr, gi = sp[1][:, :128], sp[1][:, 128:]
            fr, fi = sp[2][:, :128], sp[2][:, 128:]
            prods = (
                (vr * fr - vi * fi, vr * fi + vi * fr),
                (fr * gr + fi * gi, fr * gi - fi * gr),
                (vr * gr + vi * gi, vr * gi - vi * gr),
            )
            for n in range(3):
                qq = jnp.concatenate([prods[n][0].astype(BF), prods[n][1].astype(BF)], axis=1)
                three = jnp.dot(qq, t3_ref[...], preferred_element_type=F32)
                re, im = three[:, :128], three[:, 128:]
                p, e = ch // 2, ch % 2
                spec[n, e * 256 : e * 256 + 128, p * 128 : p * 128 + 128] = (
                    re * wr - im * wi
                ).astype(BF)
                spec[n, e * 256 + 128 : e * 256 + 256, p * 128 : p * 128 + 128] = (
                    im * wr + re * wi
                ).astype(BF)
        for n in range(3):
            four = jnp.dot(t4_ref[...], spec[n], preferred_element_type=F32)
            if n == 2:
                four = four * (1.0 / 128.0)
            for p in range(2):
                made[g, n, pair + p] = four[:, p * 128 : p * 128 + 128].astype(BF)

    lane = lax.broadcasted_iota(jnp.int32, (1, 128), 1)
    sub = lax.broadcasted_iota(jnp.int32, (8, 128), 0)

    def direct_sums(g):
        row = jnp.zeros((1, 128), F32)
        for p in range(pairs):
            terms = held[g, 0, p].astype(F32) * held[g, 1, p].astype(F32)
            folded = jnp.sum(terms.reshape(32, 8, 128), axis=0)
            for e in range(2):
                own = jnp.where(lax.rem(sub, 2) == e, folded, 0.0)
                total = jnp.sum(jnp.sum(own, axis=1, keepdims=True), axis=0, keepdims=True)
                row = row + jnp.where(lane == g * per + p * 2 + e, total, 0.0)
        sk_own[...] = sk_own[...] + row

    def send_sums():
        def one(k, carry):
            pltpu.make_async_remote_copy(
                src_ref=sk_own,
                dst_ref=sk_all.at[pl.ds(me, 1), :],
                send_sem=sk_send,
                recv_sem=sk_recv,
                device_id=target(k),
                device_id_type=MESH,
            ).start()
            return carry

        pltpu.make_async_copy(sk_own, sk_all.at[pl.ds(me, 1), :], sk_recv).start()
        lax.fori_loop(1, DEVICES, one, 0)

    def spread_sums():
        pltpu.make_async_copy(sk_all, sk_all, sk_recv).wait()
        rows = lax.broadcasted_iota(jnp.int32, (128, 128), 0)
        cols = lax.broadcasted_iota(jnp.int32, (128, 128), 1)
        mine = lax.div(cols, per) == lax.rem(rows, 16)
        for g in range(GROUPS):
            pick = (rows == g * per + lax.rem(cols, per)).astype(F32)
            wide = jnp.dot(
                sk_all[...], pick, preferred_element_type=F32, precision=lax.Precision.HIGHEST
            )
            kept = jnp.where(mine, wide, 0.0)
            sk_ref[g * 8 : g * 8 + 8, :] = jnp.sum(kept.reshape(8, 16, 128), axis=1) * (
                1.0 / 128.0
            )

    hbm_out = (lo_hbm, qg_hbm, kg_hbm, vg_hbm, fg_hbm)

    def store(n, g):
        cols = pl.ds(pl.multiple_of(g * width, width), width)
        return pltpu.make_async_copy(outs.at[n, :, cols], hbm_out[n].at[:, cols], store_sem.at[n, g])

    def finish(g):
        pltpu.make_async_copy(back.at[g], back.at[g], out_recv.at[g]).wait()

        def block(b, carry):
            cols = block_cols(g, b)
            rows = pl.ds(pl.multiple_of(b * 128, 128), 128)
            views = back.reshape(GROUPS, 3, width, 128)
            conv = views[g, 0, rows, :].T.astype(F32)
            corr = views[g, 1, rows, :].T.astype(F32)
            gain = gain_ref[pl.ds(g * (width // 128) + b, 1), :]
            kk, vv = ins[K, :, cols].astype(F32), ins[V, :, cols].astype(F32)
            gg, qq = ins[G, :, cols].astype(F32), ins[Q, :, cols].astype(F32)
            product = (kk * vv).astype(BF).astype(F32)
            mixing = conv + gain * product
            outs[0, :, cols] = (qq * mixing).astype(BF)
            outs[1, :, cols] = (gg * mixing).astype(BF)
            carried = corr + gain * (gg * qq)
            outs[2, :, cols] = (carried * vv).astype(BF)
            outs[3, :, cols] = (carried * kk).astype(BF)
            outs[4, :, cols] = views[g, 2, rows, :].T
            return carry

        lax.fori_loop(0, width // 128, block, 0)
        for n in range(5):
            store(n, g).start()

    sk_own[...] = jnp.zeros_like(sk_own)
    prepare(0)
    pl.semaphore_wait(barrier, DEVICES - 1)
    send_in(0)

    def ahead(g, carry):
        prepare(g)
        send_in(g)
        return carry

    lax.fori_loop(1, GROUPS, ahead, 0)

    for n, (source, place) in enumerate(fixed):
        pltpu.make_async_copy(source, place, table_sem.at[n]).wait()

    def middle(g, carry):
        pltpu.make_async_copy(held.at[g], held.at[g], in_recv.at[g]).wait()

        def half(h, inside):
            transform(g, h)
            return inside

        lax.fori_loop(0, pairs // 2, half, 0)
        send_out(g)
        direct_sums(g)
        return carry

    lax.fori_loop(0, GROUPS, middle, 0)
    send_sums()

    def ending(g, carry):
        finish(g)
        return carry

    lax.fori_loop(0, GROUPS - 1, ending, 0)
    spread_sums()
    finish(GROUPS - 1)
    sums_out = pltpu.make_async_copy(sk_ref, sk_hbm, table_sem.at[0])
    sums_out.start()
    everyone = held.at[:, :, :, pl.ds(0, 2 * (DEVICES - 1)), :]
    pltpu.make_async_copy(everyone, everyone, in_send).wait()
    pltpu.make_async_copy(everyone, everyone, out_send).wait()
    sums = sk_all.at[pl.ds(0, DEVICES - 1), :]
    pltpu.make_async_copy(sums, sums, sk_send).wait()
    for g in range(GROUPS):
        for n in range(5):
            store(n, g).wait()
    sums_out.wait()


def deliver(*refs):
    count = len(refs) // 2
    sem = refs[-1]
    copies = [
        pltpu.make_async_copy(refs[n], refs[count + n], sem.at[n]) for n in range(count)
    ]
    for copy in copies:
        copy.start()
    for copy in copies:
        copy.wait()


def body(query_rows, key_rows, value_rows, out_grad, filter_rows, skip_gain):
    tokens, channels = query_rows.shape
    length = tokens * DEVICES
    width = channels // GROUPS
    per = width // DEVICES
    tables = [jnp.asarray(t) for t in coefficient_tables(tokens, DEVICES, length)]
    rows = jax.ShapeDtypeStruct((tokens, channels), BF)
    anywhere = pl.BlockSpec(memory_space=pl.ANY)
    dma = pltpu.SemaphoreType.DMA
    shapes = [rows] * 5 + [jax.ShapeDtypeStruct((channels // 128, 128), F32)]
    hbm = pl.BlockSpec(memory_space=pltpu.HBM)
    results = pl.pallas_call(
        kernel,
        out_shape=shapes,
        in_specs=[hbm] * 11,
        out_specs=[anywhere] * 6,
        scratch_shapes=[
            pltpu.VMEM((channels // 128, 128), F32),
            *[pltpu.VMEM(t.shape, t.dtype) for t in tables],
            pltpu.VMEM((channels // 128, 128), F32),
            pltpu.VMEM((5, tokens, channels), BF),
            pltpu.VMEM((5, tokens, channels), BF),
            pltpu.VMEM((GROUPS, 3, width // 2, 2, 128), BF),
            pltpu.VMEM((GROUPS, 3, per // 2, 2 * DEVICES, 128), BF),
            pltpu.VMEM((GROUPS, 3, per // 2, 2 * DEVICES, 128), BF),
            pltpu.VMEM((GROUPS, 3, width // 2, 2, 128), BF),
            pltpu.VMEM((3, 4, DEVICES, 256), BF),
            pltpu.VMEM((3, 4 * DEVICES, 256), BF),
            pltpu.VMEM((1, 128), F32),
            pltpu.VMEM((DEVICES, 128), F32),
            dma((5, GROUPS)),
            dma((6,)),
            dma((5, GROUPS)),
            dma,
            dma((GROUPS,)),
            dma,
            dma((GROUPS,)),
            dma,
            dma,
        ],
        compiler_params=pltpu.CompilerParams(
            collective_id=0, has_side_effects=True, vmem_limit_bytes=36 * 1024 * 1024
        ),
        name="hyena",
    )(
        *(
            pltpu.with_memory_space_constraint(a, pltpu.HBM)
            for a in (
                query_rows,
                key_rows,
                value_rows,
                out_grad,
                filter_rows,
                skip_gain.reshape(channels // 128, 128),
                *tables,
            )
        )
    )
    results = pl.pallas_call(
        deliver,
        out_shape=shapes,
        in_specs=[anywhere] * 6,
        out_specs=[hbm] * 6,
        scratch_shapes=[dma((6,))],
        compiler_params=pltpu.CompilerParams(vmem_limit_bytes=1024 * 1024),
        name="deliver",
    )(*results)
    return (*results[:5], results[5].reshape(channels))


def solution(mesh):
    rows = P(("outer", "inner"), None)
    return jax.shard_map(
        body,
        mesh=mesh,
        in_specs=(rows, rows, rows, rows, rows, P()),
        out_specs=(rows, rows, rows, rows, rows, P()),
        check_vma=False,
    )
```

```python
import functools
import math

import jax
import jax.numpy as jnp
import numpy as np
from jax import lax
from jax.experimental import pallas as pl
from jax.experimental.pallas import tpu as pltpu
from jax.sharding import PartitionSpec as P

MESH = pl.DeviceIdType.MESH
BF = jnp.bfloat16
F32 = jnp.float32
DEVICES = 128
GROUPS = 4
ORDER = 91
VMEM_MAIN = 40
VMEM_LAST = 16


def coefficient_tables(tokens, devices, length):
    pos = np.arange(devices, dtype=np.float64)
    freq = np.arange(devices, dtype=np.float64) + 0.5
    step = np.arange(tokens, dtype=np.float64)
    one = 2.0 * np.pi * np.outer(freq, pos) / (2 * devices)
    first = np.zeros((2, 2, devices, devices, 2))
    for e in range(2):
        first[e, 0, :, :, e] = np.cos(one)
        first[e, 1, :, :, e] = -np.sin(one)
    first = first.reshape(4 * devices, 2 * devices)
    last = np.transpose(first) * (2.0 / (2 * length))
    two = 2.0 * np.pi * (np.outer(step, step) % tokens) / tokens
    c, s = np.cos(two), np.sin(two)
    forth = np.block([[c, -s], [s, c]])
    back = np.block([[c, s], [-s, c]])
    turn = 2.0 * np.pi * np.outer(freq, step) / (2 * length)
    as_bf = lambda t: np.asarray(t, np.float32).astype(jnp.bfloat16)
    return (
        as_bf(first),
        as_bf(forth),
        as_bf(back),
        as_bf(last),
        np.stack([np.cos(turn), np.sin(turn)]).astype(np.float32),
    )


def kernel(
    q_hbm,
    k_hbm,
    v_hbm,
    g_hbm,
    h_hbm,
    gain_hbm,
    t1_hbm,
    t2_hbm,
    t3_hbm,
    t4_hbm,
    tw_hbm,
    lo_ref,
    qg_ref,
    kg_ref,
    vg_ref,
    fg_ref,
    ins,
    final,
    gain_ref,
    sk_ref,
    t1_ref,
    t2_ref,
    t3_ref,
    t4_ref,
    tw_ref,
    packed,
    held,
    made,
    back,
    part,
    spec,
    sk_own,
    sk_all,
    load_sem,
    table_sem,
    in_send,
    in_recv,
    out_send,
    out_recv,
    sk_send,
    sk_recv,
):
    tokens, channels = q_hbm.shape
    width = channels // GROUPS
    per = width // DEVICES
    pairs = per // 2
    outer = lax.axis_index("outer")
    inner = lax.axis_index("inner")
    me = outer * 16 + inner
    my_y, my_zh = lax.rem(outer, 4), lax.div(outer, 4)
    my_c, my_x, my_zl = lax.rem(inner, 2), lax.rem(lax.div(inner, 2), 4), lax.div(inner, 8)
    my_z = my_zh * 2 + my_zl

    def target(k):
        j = lax.rem(k * ORDER, DEVICES)
        c = lax.rem(my_c + j, 2)
        x = lax.rem(my_x + lax.div(j, 2), 4)
        y = lax.rem(my_y + lax.div(j, 8), 4)
        z = lax.rem(my_z + lax.div(j, 32), 4)
        return lax.div(z, 2) * 4 + y, lax.rem(z, 2) * 8 + x * 2 + c

    barrier = pltpu.get_barrier_semaphore()
    row = my_x * 2 + my_c

    def greet():
        for dz in (2, 1, 3, 0):
            z = lax.rem(my_z + dz, 4)
            base = lax.rem(z, 2) * 8
            for dy in (2, 1, 3, 0):
                o = lax.div(z, 2) * 4 + lax.rem(my_y + dy, 4)
                alone = dz == 0 and dy == 0
                for t in range(1 if alone else 0, 8):
                    i = base + (lax.rem(row + t, 8) if alone else t)
                    pl.semaphore_signal(barrier, inc=1, device_id=(o, i), device_id_type=MESH)

    hbm_in = (k_hbm, v_hbm, g_hbm, q_hbm, h_hbm)
    K, V, G, Q, H = range(5)

    def load(n, g):
        cols = pl.ds(pl.multiple_of(g * width, width), width)
        return pltpu.make_async_copy(hbm_in[n].at[:, cols], ins.at[n, :, cols], load_sem.at[n, g])

    for n in range(5):
        load(n, 0).start()
    greet()
    for g in range(1, GROUPS):
        for n in range(5):
            load(n, g).start()
    fixed = (
        (t1_hbm, t1_ref),
        (t2_hbm, t2_ref),
        (t3_hbm, t3_ref),
        (t4_hbm, t4_ref),
        (tw_hbm, tw_ref),
        (gain_hbm, gain_ref),
    )
    for n, (source, place) in enumerate(fixed):
        pltpu.make_async_copy(source, place, table_sem.at[n]).start()

    def block_cols(g, b):
        return pl.ds(pl.multiple_of(g * width + b * 128, 128), 128)

    def prepare(g):
        for n in range(5):
            load(n, g).wait()

        def block(b, carry):
            cols = block_cols(g, b)
            rows = pl.ds(pl.multiple_of(b * 128, 128), 128)
            product = ins[K, :, cols].astype(F32) * ins[V, :, cols].astype(F32)
            gate = ins[G, :, cols].astype(F32) * ins[Q, :, cols].astype(F32)
            packed.reshape(GROUPS, 3, width, 128)[g, 0, rows, :] = product.astype(BF).T
            packed.reshape(GROUPS, 3, width, 128)[g, 1, rows, :] = gate.astype(BF).T
            packed.reshape(GROUPS, 3, width, 128)[g, 2, rows, :] = ins[H, :, cols].T
            return carry

        lax.fori_loop(0, width // 128, block, 0)

    def send_in(g):
        def one(k, carry):
            o, i = target(k)
            pltpu.make_async_remote_copy(
                src_ref=packed.at[g, :, pl.ds((o * 16 + i) * pairs, pairs)],
                dst_ref=held.at[g, :, :, pl.ds(me * 2, 2), :],
                send_sem=in_send,
                recv_sem=in_recv.at[g],
                device_id=(o, i),
                device_id_type=MESH,
            ).start()
            return carry

        pltpu.make_async_copy(
            packed.at[g, :, pl.ds(me * pairs, pairs)],
            held.at[g, :, :, pl.ds(me * 2, 2), :],
            in_recv.at[g],
        ).start()
        lax.fori_loop(1, DEVICES, one, 0)

    def send_out(g, place):
        def one(k, carry):
            o, i = target(k)
            pltpu.make_async_remote_copy(
                src_ref=made.at[g, :, :, pl.ds((o * 16 + i) * 2, 2), :],
                dst_ref=place.at[:, pl.ds(me * pairs, pairs)],
                send_sem=out_send,
                recv_sem=out_recv.at[g],
                device_id=(o, i),
                device_id_type=MESH,
            ).start()
            return carry

        pltpu.make_async_copy(
            made.at[g, :, :, pl.ds(me * 2, 2), :],
            place.at[:, pl.ds(me * pairs, pairs)],
            out_recv.at[g],
        ).start()
        lax.fori_loop(1, DEVICES, one, 0)

    def transform(g, h):
        wr, wi = tw_ref[0], tw_ref[1]
        pair = h * 2
        for n in range(3):
            rhs = jnp.concatenate([held[g, n, pair], held[g, n, pair + 1]], axis=1)
            one = jnp.dot(t1_ref[...], rhs, preferred_element_type=F32)
            for e in range(2):
                for p in range(2):
                    re = one[e * 256 : e * 256 + 128, p * 128 : p * 128 + 128]
                    im = one[e * 256 + 128 : e * 256 + 256, p * 128 : p * 128 + 128]
                    ch = p * 2 + e
                    part[n, ch, :, 0:128] = (re * wr + im * wi).astype(BF)
                    part[n, ch, :, 128:256] = (im * wr - re * wi).astype(BF)
        for ch in range(4):
            sp = []
            for n in range(3):
                sp.append(jnp.dot(part[n, ch], t2_ref[...], preferred_element_type=F32))
            vr, vi = sp[0][:, :128], sp[0][:, 128:]
            gr, gi = sp[1][:, :128], sp[1][:, 128:]
            fr, fi = sp[2][:, :128], sp[2][:, 128:]
            prods = (
                (vr * fr - vi * fi, vr * fi + vi * fr),
                (fr * gr + fi * gi, fr * gi - fi * gr),
                (vr * gr + vi * gi, vr * gi - vi * gr),
            )
            for n in range(3):
                qq = jnp.concatenate([prods[n][0].astype(BF), prods[n][1].astype(BF)], axis=1)
                three = jnp.dot(qq, t3_ref[...], preferred_element_type=F32)
                re, im = three[:, :128], three[:, 128:]
                p, e = ch // 2, ch % 2
                spec[n, e * 256 : e * 256 + 128, p * 128 : p * 128 + 128] = (
                    re * wr - im * wi
                ).astype(BF)
                spec[n, e * 256 + 128 : e * 256 + 256, p * 128 : p * 128 + 128] = (
                    im * wr + re * wi
                ).astype(BF)
        for n in range(3):
            four = jnp.dot(t4_ref[...], spec[n], preferred_element_type=F32)
            if n == 2:
                four = four * (1.0 / 128.0)
            for p in range(2):
                made[g, n, pair + p] = four[:, p * 128 : p * 128 + 128].astype(BF)

    lane = lax.broadcasted_iota(jnp.int32, (1, 128), 1)
    sub = lax.broadcasted_iota(jnp.int32, (8, 128), 0)

    def direct_sums(g):
        row = jnp.zeros((1, 128), F32)
        for p in range(pairs):
            terms = held[g, 0, p].astype(F32) * held[g, 1, p].astype(F32)
            folded = jnp.sum(terms.reshape(32, 8, 128), axis=0)
            for e in range(2):
                own = jnp.where(lax.rem(sub, 2) == e, folded, 0.0)
                total = jnp.sum(jnp.sum(own, axis=1, keepdims=True), axis=0, keepdims=True)
                row = row + jnp.where(lane == g * per + p * 2 + e, total, 0.0)
        sk_own[...] = sk_own[...] + row

    def send_sums():
        def one(k, carry):
            pltpu.make_async_remote_copy(
                src_ref=sk_own,
                dst_ref=sk_all.at[pl.ds(me, 1), :],
                send_sem=sk_send,
                recv_sem=sk_recv,
                device_id=target(k),
                device_id_type=MESH,
            ).start()
            return carry

        pltpu.make_async_copy(sk_own, sk_all.at[pl.ds(me, 1), :], sk_recv).start()
        lax.fori_loop(1, DEVICES, one, 0)

    def spread_sums():
        pltpu.make_async_copy(sk_all, sk_all, sk_recv).wait()
        rows = lax.broadcasted_iota(jnp.int32, (128, 128), 0)
        cols = lax.broadcasted_iota(jnp.int32, (128, 128), 1)
        mine = lax.div(cols, per) == lax.rem(rows, 16)
        for g in range(GROUPS):
            pick = (rows == g * per + lax.rem(cols, per)).astype(F32)
            wide = jnp.dot(
                sk_all[...], pick, preferred_element_type=F32, precision=lax.Precision.HIGHEST
            )
            kept = jnp.where(mine, wide, 0.0)
            sk_ref[g * 8 : g * 8 + 8, :] = jnp.sum(kept.reshape(8, 16, 128), axis=1) * (
                1.0 / 128.0
            )

    outs = (lo_ref, qg_ref, kg_ref, vg_ref, fg_ref)

    def finish(g):
        pltpu.make_async_copy(back.at[g], back.at[g], out_recv.at[g]).wait()

        def block(b, carry):
            cols = block_cols(g, b)
            rows = pl.ds(pl.multiple_of(b * 128, 128), 128)
            views = back.reshape(GROUPS - 1, 3, width, 128)
            results = results_of(
                [views[g, n, rows, :] for n in range(3)],
                [ins[n, :, cols] for n in range(4)],
                gain_ref[pl.ds(g * (width // 128) + b, 1), :],
            )
            for n in range(5):
                outs[n][:, cols] = results[n]
            return carry

        lax.fori_loop(0, width // 128, block, 0)

    sk_own[...] = jnp.zeros_like(sk_own)
    prepare(0)
    pl.semaphore_wait(barrier, DEVICES - 1)
    send_in(0)

    def ahead(g, carry):
        prepare(g)
        send_in(g)
        return carry

    lax.fori_loop(1, GROUPS, ahead, 0)

    for n, (source, place) in enumerate(fixed):
        pltpu.make_async_copy(source, place, table_sem.at[n]).wait()

    def middle(g, carry):
        pltpu.make_async_copy(held.at[g], held.at[g], in_recv.at[g]).wait()

        def half(h, inside):
            transform(g, h)
            return inside

        direct_sums(g)

        @pl.when(g == GROUPS - 1)
        def _():
            send_sums()

        lax.fori_loop(0, pairs // 2, half, 0)

        @pl.when(g < GROUPS - 1)
        def _():
            send_out(g, back.at[g])

        @pl.when(g == GROUPS - 1)
        def _():
            send_out(g, final)

        return carry

    lax.fori_loop(0, GROUPS, middle, 0)

    def ending(g, carry):
        finish(g)
        return carry

    lax.fori_loop(0, GROUPS - 1, ending, 0)
    spread_sums()
    everyone = held.at[:, :, :, pl.ds(0, 2 * (DEVICES - 1)), :]
    pltpu.make_async_copy(everyone, everyone, in_send).wait()
    sums = sk_all.at[pl.ds(0, DEVICES - 1), :]
    pltpu.make_async_copy(sums, sums, sk_send).wait()
    pltpu.make_async_copy(final, final, out_recv.at[GROUPS - 1]).wait()
    pltpu.make_async_copy(everyone, everyone, out_send).wait()


def results_of(sums, rows, gain):
    conv, corr = sums[0].T.astype(F32), sums[1].T.astype(F32)
    kk, vv, gg, qq = (r.astype(F32) for r in rows)
    product = (kk * vv).astype(BF).astype(F32)
    mixing = conv + gain * product
    carried = corr + gain * (gg * qq)
    return (
        (qq * mixing).astype(BF),
        (gg * mixing).astype(BF),
        (carried * vv).astype(BF),
        (carried * kk).astype(BF),
        sums[2].T,
    )


def deliver(*refs):
    early, (ins, final, gain_ref, sums) = refs[:5], refs[5:9]
    whole, sums_out = refs[9:14], refs[14]
    late, sem = refs[15], refs[16]
    channels = whole[0].shape[1]
    width = channels // GROUPS
    first = channels - width
    parts = 2
    step = width // parts
    copies = [
        pltpu.make_async_copy(early[n], whole[n].at[:, pl.ds(0, first)], sem.at[n])
        for n in range(5)
    ]
    copies.append(pltpu.make_async_copy(sums, sums_out, sem.at[5]))
    for copy in copies:
        copy.start()
    views = final.reshape(3, width, 128)
    for part in range(parts):

        def block(b, carry):
            at = pl.multiple_of(part * step + b * 128, 128)
            cols = pl.ds(first + at, 128)
            results = results_of(
                [views[n, pl.ds(at, 128), :] for n in range(3)],
                [ins[n, :, cols] for n in range(4)],
                gain_ref[pl.ds((first + part * step) // 128 + b, 1), :],
            )
            for n in range(5):
                late[n, :, pl.ds(at, 128)] = results[n]
            return carry

        lax.fori_loop(0, step // 128, block, 0)
        for n in range(5):
            copies.append(
                pltpu.make_async_copy(
                    late.at[n, :, pl.ds(part * step, step)],
                    whole[n].at[:, pl.ds(first + part * step, step)],
                    sem.at[6 + part * 5 + n],
                )
            )
            copies[-1].start()
    for copy in copies:
        copy.wait()


def body(query_rows, key_rows, value_rows, out_grad, filter_rows, skip_gain):
    tokens, channels = query_rows.shape
    length = tokens * DEVICES
    width = channels // GROUPS
    per = width // DEVICES
    tables = [jnp.asarray(t) for t in coefficient_tables(tokens, DEVICES, length)]
    rows = jax.ShapeDtypeStruct((tokens, channels), BF)
    anywhere = pl.BlockSpec(memory_space=pl.ANY)
    dma = pltpu.SemaphoreType.DMA
    sums = jax.ShapeDtypeStruct((channels // 128, 128), F32)
    early = jax.ShapeDtypeStruct((tokens, channels - width), BF)
    hbm = pl.BlockSpec(memory_space=pltpu.HBM)
    vmem = pl.BlockSpec(memory_space=pltpu.VMEM)
    handed = pl.pallas_call(
        kernel,
        out_shape=[early] * 5
        + [
            jax.ShapeDtypeStruct((5, tokens, channels), BF),
            jax.ShapeDtypeStruct((3, width // 2, 2, 128), BF),
            sums,
            sums,
        ],
        in_specs=[hbm] * 11,
        out_specs=[vmem] * 9,
        scratch_shapes=[
            *[pltpu.VMEM(t.shape, t.dtype) for t in tables],
            pltpu.VMEM((GROUPS, 3, width // 2, 2, 128), BF),
            pltpu.VMEM((GROUPS, 3, per // 2, 2 * DEVICES, 128), BF),
            pltpu.VMEM((GROUPS, 3, per // 2, 2 * DEVICES, 128), BF),
            pltpu.VMEM((GROUPS - 1, 3, width // 2, 2, 128), BF),
            pltpu.VMEM((3, 4, DEVICES, 256), BF),
            pltpu.VMEM((3, 4 * DEVICES, 256), BF),
            pltpu.VMEM((1, 128), F32),
            pltpu.VMEM((DEVICES, 128), F32),
            dma((5, GROUPS)),
            dma((6,)),
            dma,
            dma((GROUPS,)),
            dma,
            dma((GROUPS,)),
            dma,
            dma,
        ],
        compiler_params=pltpu.CompilerParams(
            collective_id=0, has_side_effects=True, vmem_limit_bytes=VMEM_MAIN * 1024 * 1024
        ),
        name="hyena",
    )(
        *(
            pltpu.with_memory_space_constraint(a, pltpu.HBM)
            for a in (
                query_rows,
                key_rows,
                value_rows,
                out_grad,
                filter_rows,
                skip_gain.reshape(channels // 128, 128),
                *tables,
            )
        )
    )
    results = pl.pallas_call(
        deliver,
        out_shape=[rows] * 5 + [sums],
        in_specs=[anywhere] * 5 + [vmem] * 3 + [anywhere],
        out_specs=[hbm] * 6,
        scratch_shapes=[pltpu.VMEM((5, tokens, width), BF), dma((16,))],
        compiler_params=pltpu.CompilerParams(vmem_limit_bytes=VMEM_LAST * 1024 * 1024),
        name="deliver",
    )(*handed)
    return (*results[:5], results[5].reshape(channels))


def solution(mesh):
    rows = P(("outer", "inner"), None)
    return jax.shard_map(
        body,
        mesh=mesh,
        in_specs=(rows, rows, rows, rows, rows, P()),
        out_specs=(rows, rows, rows, rows, rows, P()),
        check_vma=False,
    )
```

```python
import functools
import math

import jax
import jax.numpy as jnp
import numpy as np
from jax import lax
from jax.experimental import pallas as pl
from jax.experimental.pallas import tpu as pltpu
from jax.sharding import PartitionSpec as P

MESH = pl.DeviceIdType.MESH
BF = jnp.bfloat16
F32 = jnp.float32
DEVICES = 128
GROUPS = 4
ORDER = 91
VMEM_MAIN = 40
VMEM_LAST = 16


def coefficient_tables(tokens, devices, length):
    pos = np.arange(devices, dtype=np.float64)
    freq = np.arange(devices, dtype=np.float64) + 0.5
    step = np.arange(tokens, dtype=np.float64)
    one = 2.0 * np.pi * np.outer(freq, pos) / (2 * devices)
    first = np.zeros((2, 2, devices, devices, 2))
    for e in range(2):
        first[e, 0, :, :, e] = np.cos(one)
        first[e, 1, :, :, e] = -np.sin(one)
    first = first.reshape(4 * devices, 2 * devices)
    last = np.transpose(first) * (2.0 / (2 * length))
    two = 2.0 * np.pi * (np.outer(step, step) % tokens) / tokens
    c, s = np.cos(two), np.sin(two)
    forth = np.block([[c, -s], [s, c]])
    back = np.block([[c, s], [-s, c]])
    turn = 2.0 * np.pi * np.outer(freq, step) / (2 * length)
    as_bf = lambda t: np.asarray(t, np.float32).astype(jnp.bfloat16)
    return (
        as_bf(first),
        as_bf(forth),
        as_bf(back),
        as_bf(last),
        np.stack([np.cos(turn), np.sin(turn)]).astype(np.float32),
    )


def kernel(
    q_hbm,
    k_hbm,
    v_hbm,
    g_hbm,
    h_hbm,
    gain_hbm,
    t1_hbm,
    t2_hbm,
    t3_hbm,
    t4_hbm,
    tw_hbm,
    lo_ref,
    qg_ref,
    kg_ref,
    vg_ref,
    fg_ref,
    ins,
    final,
    gain_ref,
    sk_ref,
    t1_ref,
    t2_ref,
    t3_ref,
    t4_ref,
    tw_ref,
    packed,
    held,
    made,
    back,
    part,
    spec,
    sk_own,
    sk_near,
    sk_row,
    sk_all,
    load_sem,
    table_sem,
    in_send,
    in_recv,
    out_send,
    out_recv,
    sk_send,
    sk_recv,
    near_send,
    near_recv,
):
    tokens, channels = q_hbm.shape
    width = channels // GROUPS
    per = width // DEVICES
    pairs = per // 2
    outer = lax.axis_index("outer")
    inner = lax.axis_index("inner")
    me = outer * 16 + inner
    my_y, my_zh = lax.rem(outer, 4), lax.div(outer, 4)
    my_c, my_x, my_zl = lax.rem(inner, 2), lax.rem(lax.div(inner, 2), 4), lax.div(inner, 8)
    my_z = my_zh * 2 + my_zl

    def target(k):
        j = lax.rem(k * ORDER, DEVICES)
        c = lax.rem(my_c + j, 2)
        x = lax.rem(my_x + lax.div(j, 2), 4)
        y = lax.rem(my_y + lax.div(j, 8), 4)
        z = lax.rem(my_z + lax.div(j, 32), 4)
        return lax.div(z, 2) * 4 + y, lax.rem(z, 2) * 8 + x * 2 + c

    barrier = pltpu.get_barrier_semaphore()
    row = my_x * 2 + my_c

    def greet():
        for dz in (2, 1, 3, 0):
            z = lax.rem(my_z + dz, 4)
            base = lax.rem(z, 2) * 8
            for dy in (2, 1, 3, 0):
                o = lax.div(z, 2) * 4 + lax.rem(my_y + dy, 4)
                alone = dz == 0 and dy == 0
                for t in range(1 if alone else 0, 8):
                    i = base + (lax.rem(row + t, 8) if alone else t)
                    pl.semaphore_signal(barrier, inc=1, device_id=(o, i), device_id_type=MESH)

    hbm_in = (k_hbm, v_hbm, g_hbm, q_hbm, h_hbm)
    K, V, G, Q, H = range(5)

    def load(n, g):
        cols = pl.ds(pl.multiple_of(g * width, width), width)
        return pltpu.make_async_copy(hbm_in[n].at[:, cols], ins.at[n, :, cols], load_sem.at[n, g])

    for n in range(5):
        load(n, 0).start()
    greet()
    for g in range(1, GROUPS):
        for n in range(5):
            load(n, g).start()
    fixed = (
        (t1_hbm, t1_ref),
        (t2_hbm, t2_ref),
        (t3_hbm, t3_ref),
        (t4_hbm, t4_ref),
        (tw_hbm, tw_ref),
        (gain_hbm, gain_ref),
    )
    for n, (source, place) in enumerate(fixed):
        pltpu.make_async_copy(source, place, table_sem.at[n]).start()

    def block_cols(g, b):
        return pl.ds(pl.multiple_of(g * width + b * 128, 128), 128)

    def prepare(g):
        for n in range(5):
            load(n, g).wait()

        def block(b, carry):
            cols = block_cols(g, b)
            rows = pl.ds(pl.multiple_of(b * 128, 128), 128)
            product = ins[K, :, cols].astype(F32) * ins[V, :, cols].astype(F32)
            gate = ins[G, :, cols].astype(F32) * ins[Q, :, cols].astype(F32)
            packed.reshape(GROUPS, 3, width, 128)[g, 0, rows, :] = product.astype(BF).T
            packed.reshape(GROUPS, 3, width, 128)[g, 1, rows, :] = gate.astype(BF).T
            packed.reshape(GROUPS, 3, width, 128)[g, 2, rows, :] = ins[H, :, cols].T
            return carry

        lax.fori_loop(0, width // 128, block, 0)

    def send_in(g):
        def one(k, carry):
            o, i = target(k)
            pltpu.make_async_remote_copy(
                src_ref=packed.at[g, :, pl.ds((o * 16 + i) * pairs, pairs)],
                dst_ref=held.at[g, :, :, pl.ds(me * 2, 2), :],
                send_sem=in_send,
                recv_sem=in_recv.at[g],
                device_id=(o, i),
                device_id_type=MESH,
            ).start()
            return carry

        pltpu.make_async_copy(
            packed.at[g, :, pl.ds(me * pairs, pairs)],
            held.at[g, :, :, pl.ds(me * 2, 2), :],
            in_recv.at[g],
        ).start()
        lax.fori_loop(1, DEVICES, one, 0)

    def hops(k):
        j = lax.rem(k * ORDER, DEVICES)
        total = 0
        for d in (lax.rem(lax.div(j, 2), 4), lax.rem(lax.div(j, 8), 4), lax.div(j, 32)):
            total = total + jnp.minimum(d, 4 - d)
        return total

    def send_out(g, place, far_first=False):
        def one(k, carry):
            o, i = target(k)
            pltpu.make_async_remote_copy(
                src_ref=made.at[g, :, :, pl.ds((o * 16 + i) * 2, 2), :],
                dst_ref=place.at[:, pl.ds(me * pairs, pairs)],
                send_sem=out_send,
                recv_sem=out_recv.at[g],
                device_id=(o, i),
                device_id_type=MESH,
            ).start()
            return carry

        def far(k, carry):
            @pl.when(hops(k) > 2)
            def _():
                one(k, 0)

            return carry

        def near(k, carry):
            @pl.when(hops(k) <= 2)
            def _():
                one(k, 0)

            return carry

        pltpu.make_async_copy(
            made.at[g, :, :, pl.ds(me * 2, 2), :],
            place.at[:, pl.ds(me * pairs, pairs)],
            out_recv.at[g],
        ).start()
        if far_first:
            lax.fori_loop(1, DEVICES, far, 0)
            lax.fori_loop(1, DEVICES, near, 0)
        else:
            lax.fori_loop(1, DEVICES, one, 0)

    def transform(g, h):
        wr, wi = tw_ref[0], tw_ref[1]
        pair = h * 2
        for n in range(3):
            rhs = jnp.concatenate([held[g, n, pair], held[g, n, pair + 1]], axis=1)
            one = jnp.dot(t1_ref[...], rhs, preferred_element_type=F32)
            for e in range(2):
                for p in range(2):
                    re = one[e * 256 : e * 256 + 128, p * 128 : p * 128 + 128]
                    im = one[e * 256 + 128 : e * 256 + 256, p * 128 : p * 128 + 128]
                    ch = p * 2 + e
                    part[n, ch, :, 0:128] = (re * wr + im * wi).astype(BF)
                    part[n, ch, :, 128:256] = (im * wr - re * wi).astype(BF)
        for ch in range(4):
            sp = []
            for n in range(3):
                sp.append(jnp.dot(part[n, ch], t2_ref[...], preferred_element_type=F32))
            vr, vi = sp[0][:, :128], sp[0][:, 128:]
            gr, gi = sp[1][:, :128], sp[1][:, 128:]
            fr, fi = sp[2][:, :128], sp[2][:, 128:]
            prods = (
                (vr * fr - vi * fi, vr * fi + vi * fr),
                (fr * gr + fi * gi, fr * gi - fi * gr),
                (vr * gr + vi * gi, vr * gi - vi * gr),
            )
            for n in range(3):
                qq = jnp.concatenate([prods[n][0].astype(BF), prods[n][1].astype(BF)], axis=1)
                three = jnp.dot(qq, t3_ref[...], preferred_element_type=F32)
                re, im = three[:, :128], three[:, 128:]
                p, e = ch // 2, ch % 2
                spec[n, e * 256 : e * 256 + 128, p * 128 : p * 128 + 128] = (
                    re * wr - im * wi
                ).astype(BF)
                spec[n, e * 256 + 128 : e * 256 + 256, p * 128 : p * 128 + 128] = (
                    im * wr + re * wi
                ).astype(BF)
        for n in range(3):
            four = jnp.dot(t4_ref[...], spec[n], preferred_element_type=F32)
            if n == 2:
                four = four * (1.0 / 128.0)
            for p in range(2):
                made[g, n, pair + p] = four[:, p * 128 : p * 128 + 128].astype(BF)

    lane = lax.broadcasted_iota(jnp.int32, (1, 128), 1)
    sub = lax.broadcasted_iota(jnp.int32, (8, 128), 0)

    def direct_sums(g):
        row = jnp.zeros((1, 128), F32)
        for p in range(pairs):
            terms = held[g, 0, p].astype(F32) * held[g, 1, p].astype(F32)
            folded = jnp.sum(terms.reshape(32, 8, 128), axis=0)
            for e in range(2):
                own = jnp.where(lax.rem(sub, 2) == e, folded, 0.0)
                total = jnp.sum(jnp.sum(own, axis=1, keepdims=True), axis=0, keepdims=True)
                row = row + jnp.where(lane == g * per + p * 2 + e, total, 0.0)
        sk_own[...] = sk_own[...] + row

    def send_sums():
        own = sk_own[...]
        spread = own
        for n in range(1, 4):
            spread = jnp.where(lax.div(lane, per * GROUPS) == n, pltpu.roll(own, n * per * GROUPS, 1), spread)
        sk_own[...] = jnp.where(lax.div(lane, per * GROUPS) == lax.rem(row, 4), spread, 0.0)
        pltpu.make_async_copy(sk_own, sk_near.at[pl.ds(row, 1), :], near_recv).start()
        for t in range(1, 8):
            pltpu.make_async_remote_copy(
                src_ref=sk_own,
                dst_ref=sk_near.at[pl.ds(row, 1), :],
                send_sem=near_send,
                recv_sem=near_recv,
                device_id=(outer, my_zl * 8 + lax.rem(row + t, 8)),
                device_id_type=MESH,
            ).start()

    def pass_sums():
        pltpu.make_async_copy(sk_near, sk_near, near_recv).wait()
        sk_row[...] = jnp.sum(sk_near[...].reshape(2, 4, 128), axis=1)
        mine = outer * 2 + my_zl
        pltpu.make_async_copy(sk_row, sk_all.at[mine], sk_recv).start()
        for dz in (2, 1, 3, 0):
            z = lax.rem(my_z + dz, 4)
            for dy in (2, 1, 3, 0):
                if dz or dy:
                    o = lax.div(z, 2) * 4 + lax.rem(my_y + dy, 4)
                    pltpu.make_async_remote_copy(
                        src_ref=sk_row,
                        dst_ref=sk_all.at[mine],
                        send_sem=sk_send,
                        recv_sem=sk_recv,
                        device_id=(o, lax.rem(z, 2) * 8 + row),
                        device_id_type=MESH,
                    ).start()

    def spread_sums():
        pltpu.make_async_copy(sk_all, sk_all, sk_recv).wait()
        gathered = sk_all[...].reshape(32, 128)
        rows = lax.broadcasted_iota(jnp.int32, (32, 128), 0)
        cols = lax.broadcasted_iota(jnp.int32, (32, 128), 1)
        mine = lax.div(cols, 32) == lax.rem(rows, 4)
        source = lax.broadcasted_iota(jnp.int32, (128, 128), 0)
        place = lax.broadcasted_iota(jnp.int32, (128, 128), 1)
        base = lax.rem(lax.div(place, per), 4) * (per * GROUPS) + lax.rem(place, per)
        for g in range(GROUPS):
            pick = (source == base + g * per).astype(F32)
            wide = jnp.dot(
                gathered, pick, preferred_element_type=F32, precision=lax.Precision.HIGHEST
            )
            kept = jnp.where(mine, wide, 0.0)
            sk_ref[g * 8 : g * 8 + 8, :] = jnp.sum(kept.reshape(8, 4, 128), axis=1) * (
                1.0 / 128.0
            )

    outs = (lo_ref, qg_ref, kg_ref, vg_ref, fg_ref)

    def finish(g):
        pltpu.make_async_copy(back.at[g], back.at[g], out_recv.at[g]).wait()

        def block(b, carry):
            cols = block_cols(g, b)
            rows = pl.ds(pl.multiple_of(b * 128, 128), 128)
            views = back.reshape(GROUPS - 1, 3, width, 128)
            results = results_of(
                [views[g, n, rows, :] for n in range(3)],
                [ins[n, :, cols] for n in range(4)],
                gain_ref[pl.ds(g * (width // 128) + b, 1), :],
            )
            for n in range(5):
                outs[n][:, cols] = results[n]
            return carry

        lax.fori_loop(0, width // 128, block, 0)

    sk_own[...] = jnp.zeros_like(sk_own)
    prepare(0)
    pl.semaphore_wait(barrier, DEVICES - 1)
    send_in(0)

    def ahead(g, carry):
        prepare(g)
        send_in(g)
        return carry

    lax.fori_loop(1, GROUPS, ahead, 0)

    for n, (source, place) in enumerate(fixed):
        pltpu.make_async_copy(source, place, table_sem.at[n]).wait()

    def middle(g, carry):
        pltpu.make_async_copy(held.at[g], held.at[g], in_recv.at[g]).wait()

        def half(h, inside):
            transform(g, h)
            return inside

        direct_sums(g)

        @pl.when(g == GROUPS - 1)
        def _():
            send_sums()

        lax.fori_loop(0, pairs // 2, half, 0)

        @pl.when(g < GROUPS - 1)
        def _():
            send_out(g, back.at[g])

        @pl.when(g == GROUPS - 1)
        def _():
            send_out(g, final, far_first=True)

        return carry

    lax.fori_loop(0, GROUPS, middle, 0)

    def ending(g, carry):
        finish(g)
        return carry

    lax.fori_loop(0, GROUPS - 2, ending, 0)
    pass_sums()
    finish(GROUPS - 2)
    spread_sums()
    everyone = held.at[:, :, :, pl.ds(0, 2 * (DEVICES - 1)), :]
    pltpu.make_async_copy(everyone, everyone, in_send).wait()
    near = sk_near.at[pl.ds(0, 7), :]
    pltpu.make_async_copy(near, near, near_send).wait()
    sums = sk_all.at[pl.ds(0, 15)]
    pltpu.make_async_copy(sums, sums, sk_send).wait()
    pltpu.make_async_copy(final, final, out_recv.at[GROUPS - 1]).wait()
    pltpu.make_async_copy(everyone, everyone, out_send).wait()


def results_of(sums, rows, gain):
    conv, corr = sums[0].T.astype(F32), sums[1].T.astype(F32)
    kk, vv, gg, qq = (r.astype(F32) for r in rows)
    product = (kk * vv).astype(BF).astype(F32)
    mixing = conv + gain * product
    carried = corr + gain * (gg * qq)
    return (
        (qq * mixing).astype(BF),
        (gg * mixing).astype(BF),
        (carried * vv).astype(BF),
        (carried * kk).astype(BF),
        sums[2].T,
    )


def deliver(*refs):
    early, (ins, final, gain_ref, sums) = refs[:5], refs[5:9]
    whole, sums_out = refs[9:14], refs[14]
    late, sem = refs[15], refs[16]
    channels = whole[0].shape[1]
    width = channels // GROUPS
    first = channels - width
    parts = 2
    step = width // parts
    copies = [
        pltpu.make_async_copy(early[n], whole[n].at[:, pl.ds(0, first)], sem.at[n])
        for n in range(5)
    ]
    copies.append(pltpu.make_async_copy(sums, sums_out, sem.at[5]))
    for copy in copies:
        copy.start()
    views = final.reshape(3, width, 128)
    for part in range(parts):

        def block(b, carry):
            at = pl.multiple_of(part * step + b * 128, 128)
            cols = pl.ds(first + at, 128)
            results = results_of(
                [views[n, pl.ds(at, 128), :] for n in range(3)],
                [ins[n, :, cols] for n in range(4)],
                gain_ref[pl.ds((first + part * step) // 128 + b, 1), :],
            )
            for n in range(5):
                late[n, :, pl.ds(at, 128)] = results[n]
            return carry

        lax.fori_loop(0, step // 128, block, 0)
        for n in range(5):
            copies.append(
                pltpu.make_async_copy(
                    late.at[n, :, pl.ds(part * step, step)],
                    whole[n].at[:, pl.ds(first + part * step, step)],
                    sem.at[6 + part * 5 + n],
                )
            )
            copies[-1].start()
    for copy in copies:
        copy.wait()


def body(query_rows, key_rows, value_rows, out_grad, filter_rows, skip_gain):
    tokens, channels = query_rows.shape
    length = tokens * DEVICES
    width = channels // GROUPS
    per = width // DEVICES
    tables = [jnp.asarray(t) for t in coefficient_tables(tokens, DEVICES, length)]
    rows = jax.ShapeDtypeStruct((tokens, channels), BF)
    anywhere = pl.BlockSpec(memory_space=pl.ANY)
    dma = pltpu.SemaphoreType.DMA
    sums = jax.ShapeDtypeStruct((channels // 128, 128), F32)
    early = jax.ShapeDtypeStruct((tokens, channels - width), BF)
    hbm = pl.BlockSpec(memory_space=pltpu.HBM)
    vmem = pl.BlockSpec(memory_space=pltpu.VMEM)
    handed = pl.pallas_call(
        kernel,
        out_shape=[early] * 5
        + [
            jax.ShapeDtypeStruct((5, tokens, channels), BF),
            jax.ShapeDtypeStruct((3, width // 2, 2, 128), BF),
            sums,
            sums,
        ],
        in_specs=[hbm] * 11,
        out_specs=[vmem] * 9,
        scratch_shapes=[
            *[pltpu.VMEM(t.shape, t.dtype) for t in tables],
            pltpu.VMEM((GROUPS, 3, width // 2, 2, 128), BF),
            pltpu.VMEM((GROUPS, 3, per // 2, 2 * DEVICES, 128), BF),
            pltpu.VMEM((GROUPS, 3, per // 2, 2 * DEVICES, 128), BF),
            pltpu.VMEM((GROUPS - 1, 3, width // 2, 2, 128), BF),
            pltpu.VMEM((3, 4, DEVICES, 256), BF),
            pltpu.VMEM((3, 4 * DEVICES, 256), BF),
            pltpu.VMEM((1, 128), F32),
            pltpu.VMEM((8, 128), F32),
            pltpu.VMEM((2, 128), F32),
            pltpu.VMEM((16, 2, 128), F32),
            dma((5, GROUPS)),
            dma((6,)),
            dma,
            dma((GROUPS,)),
            dma,
            dma((GROUPS,)),
            dma,
            dma,
            dma,
            dma,
        ],
        compiler_params=pltpu.CompilerParams(
            collective_id=0, has_side_effects=True, vmem_limit_bytes=VMEM_MAIN * 1024 * 1024
        ),
        name="hyena",
    )(
        *(
            pltpu.with_memory_space_constraint(a, pltpu.HBM)
            for a in (
                query_rows,
                key_rows,
                value_rows,
                out_grad,
                filter_rows,
                skip_gain.reshape(channels // 128, 128),
                *tables,
            )
        )
    )
    results = pl.pallas_call(
        deliver,
        out_shape=[rows] * 5 + [sums],
        in_specs=[anywhere] * 5 + [vmem] * 3 + [anywhere],
        out_specs=[hbm] * 6,
        scratch_shapes=[pltpu.VMEM((5, tokens, width), BF), dma((16,))],
        compiler_params=pltpu.CompilerParams(vmem_limit_bytes=VMEM_LAST * 1024 * 1024),
        name="deliver",
    )(*handed)
    return (*results[:5], results[5].reshape(channels))


def solution(mesh):
    rows = P(("outer", "inner"), None)
    return jax.shard_map(
        body,
        mesh=mesh,
        in_specs=(rows, rows, rows, rows, rows, P()),
        out_specs=(rows, rows, rows, rows, rows, P()),
        check_vma=False,
    )
```

```python
import functools
import math

import jax
import jax.numpy as jnp
import numpy as np
from jax import lax
from jax.experimental import pallas as pl
from jax.experimental.pallas import tpu as pltpu
from jax.sharding import PartitionSpec as P

MESH = pl.DeviceIdType.MESH
BF = jnp.bfloat16
F32 = jnp.float32
DEVICES = 128
GROUPS = 4
ORDER = 91
VMEM_MAIN = 40
VMEM_LAST = 16


def coefficient_tables(tokens, devices, length):
    pos = np.arange(devices, dtype=np.float64)
    freq = np.arange(devices, dtype=np.float64) + 0.5
    step = np.arange(tokens, dtype=np.float64)
    one = 2.0 * np.pi * np.outer(freq, pos) / (2 * devices)
    first = np.zeros((2, 2, devices, devices, 2))
    for e in range(2):
        first[e, 0, :, :, e] = np.cos(one)
        first[e, 1, :, :, e] = -np.sin(one)
    first = first.reshape(4 * devices, 2 * devices)
    last = np.transpose(first) * (2.0 / (2 * length))
    two = 2.0 * np.pi * (np.outer(step, step) % tokens) / tokens
    c, s = np.cos(two), np.sin(two)
    forth = np.block([[c, -s], [s, c]])
    back = np.block([[c, s], [-s, c]])
    turn = 2.0 * np.pi * np.outer(freq, step) / (2 * length)
    as_bf = lambda t: np.asarray(t, np.float32).astype(jnp.bfloat16)
    return (
        as_bf(first),
        as_bf(forth),
        as_bf(back),
        as_bf(last),
        np.stack([np.cos(turn), np.sin(turn)]).astype(np.float32),
    )


def kernel(
    q_hbm,
    k_hbm,
    v_hbm,
    g_hbm,
    h_hbm,
    gain_hbm,
    t1_hbm,
    t2_hbm,
    t3_hbm,
    t4_hbm,
    tw_hbm,
    lo_ref,
    qg_ref,
    kg_ref,
    vg_ref,
    fg_ref,
    ins,
    final,
    gain_ref,
    sk_ref,
    t1_ref,
    t2_ref,
    t3_ref,
    t4_ref,
    tw_ref,
    packed,
    held,
    made,
    back,
    part,
    spec,
    sk_own,
    sk_near,
    sk_row,
    sk_all,
    load_sem,
    table_sem,
    in_send,
    in_recv,
    out_send,
    out_recv,
    sk_send,
    sk_recv,
    near_send,
    near_recv,
):
    tokens, channels = q_hbm.shape
    width = channels // GROUPS
    per = width // DEVICES
    pairs = per // 2
    outer = lax.axis_index("outer")
    inner = lax.axis_index("inner")
    me = outer * 16 + inner
    my_y, my_zh = lax.rem(outer, 4), lax.div(outer, 4)
    my_c, my_x, my_zl = lax.rem(inner, 2), lax.rem(lax.div(inner, 2), 4), lax.div(inner, 8)
    my_z = my_zh * 2 + my_zl

    def target(k):
        j = lax.rem(k * ORDER, DEVICES)
        c = lax.rem(my_c + j, 2)
        x = lax.rem(my_x + lax.div(j, 2), 4)
        y = lax.rem(my_y + lax.div(j, 8), 4)
        z = lax.rem(my_z + lax.div(j, 32), 4)
        return lax.div(z, 2) * 4 + y, lax.rem(z, 2) * 8 + x * 2 + c

    barrier = pltpu.get_barrier_semaphore()
    row = my_x * 2 + my_c

    def greet():
        for dz in (2, 1, 3, 0):
            z = lax.rem(my_z + dz, 4)
            base = lax.rem(z, 2) * 8
            for dy in (2, 1, 3, 0):
                o = lax.div(z, 2) * 4 + lax.rem(my_y + dy, 4)
                alone = dz == 0 and dy == 0
                for t in range(1 if alone else 0, 8):
                    i = base + (lax.rem(row + t, 8) if alone else t)
                    pl.semaphore_signal(barrier, inc=1, device_id=(o, i), device_id_type=MESH)

    hbm_in = (k_hbm, v_hbm, g_hbm, q_hbm, h_hbm)
    K, V, G, Q, H = range(5)

    def load(n, g):
        cols = pl.ds(pl.multiple_of(g * width, width), width)
        return pltpu.make_async_copy(hbm_in[n].at[:, cols], ins.at[n, :, cols], load_sem.at[n, g])

    for n in range(5):
        load(n, 0).start()
    greet()
    for g in range(1, GROUPS):
        for n in range(5):
            load(n, g).start()
    fixed = (
        (t1_hbm, t1_ref),
        (t2_hbm, t2_ref),
        (t3_hbm, t3_ref),
        (t4_hbm, t4_ref),
        (tw_hbm, tw_ref),
        (gain_hbm, gain_ref),
    )
    for n, (source, place) in enumerate(fixed):
        pltpu.make_async_copy(source, place, table_sem.at[n]).start()

    def block_cols(g, b):
        return pl.ds(pl.multiple_of(g * width + b * 128, 128), 128)

    def prepare(g):
        for n in range(5):
            load(n, g).wait()

        def block(b, carry):
            cols = block_cols(g, b)
            rows = pl.ds(pl.multiple_of(b * 128, 128), 128)
            product = ins[K, :, cols].astype(F32) * ins[V, :, cols].astype(F32)
            gate = ins[G, :, cols].astype(F32) * ins[Q, :, cols].astype(F32)
            packed.reshape(GROUPS, 3, width, 128)[g, 0, rows, :] = product.astype(BF).T
            packed.reshape(GROUPS, 3, width, 128)[g, 1, rows, :] = gate.astype(BF).T
            packed.reshape(GROUPS, 3, width, 128)[g, 2, rows, :] = ins[H, :, cols].T
            return carry

        lax.fori_loop(0, width // 128, block, 0)

    def send_in(g):
        def one(k, carry):
            o, i = target(k)
            pltpu.make_async_remote_copy(
                src_ref=packed.at[g, :, pl.ds((o * 16 + i) * pairs, pairs)],
                dst_ref=held.at[g, :, :, pl.ds(me * 2, 2), :],
                send_sem=in_send,
                recv_sem=in_recv.at[g],
                device_id=(o, i),
                device_id_type=MESH,
            ).start()
            return carry

        pltpu.make_async_copy(
            packed.at[g, :, pl.ds(me * pairs, pairs)],
            held.at[g, :, :, pl.ds(me * 2, 2), :],
            in_recv.at[g],
        ).start()
        lax.fori_loop(1, DEVICES, one, 0)

    o_z = [lax.div(lax.rem(my_z + d, 4), 2) * 4 for d in range(4)]
    i_z = [lax.rem(lax.rem(my_z + d, 4), 2) * 8 for d in range(4)]
    o_y = [lax.rem(my_y + d, 4) for d in range(4)]
    i_x = [lax.rem(my_x + d, 4) * 2 for d in range(4)]
    i_c = [my_c, 1 - my_c]

    def at_offset(c, x, y, z):
        return o_z[z] + o_y[y], i_z[z] + i_x[x] + i_c[c]

    offsets = [
        (j % 2, j // 2 % 4, j // 8 % 4, j // 32)
        for j in (k * ORDER % DEVICES for k in range(1, DEVICES))
    ]

    def hops(offset):
        return sum(min(d, 4 - d) for d in offset[1:])

    def send_out(g, place, far_first=False):
        def to(o, i):
            pltpu.make_async_remote_copy(
                src_ref=made.at[g, :, :, pl.ds((o * 16 + i) * 2, 2), :],
                dst_ref=place.at[:, pl.ds(me * pairs, pairs)],
                send_sem=out_send,
                recv_sem=out_recv.at[g],
                device_id=(o, i),
                device_id_type=MESH,
            ).start()

        def one(k, carry):
            to(*target(k))
            return carry

        pltpu.make_async_copy(
            made.at[g, :, :, pl.ds(me * 2, 2), :],
            place.at[:, pl.ds(me * pairs, pairs)],
            out_recv.at[g],
        ).start()
        if far_first:
            for offset in sorted(offsets, key=lambda f: hops(f) <= 2):
                to(*at_offset(*offset))
        else:
            lax.fori_loop(1, DEVICES, one, 0)

    def transform(g, h):
        wr, wi = tw_ref[0], tw_ref[1]
        pair = h * 2
        for n in range(3):
            rhs = jnp.concatenate([held[g, n, pair], held[g, n, pair + 1]], axis=1)
            one = jnp.dot(t1_ref[...], rhs, preferred_element_type=F32)
            for e in range(2):
                for p in range(2):
                    re = one[e * 256 : e * 256 + 128, p * 128 : p * 128 + 128]
                    im = one[e * 256 + 128 : e * 256 + 256, p * 128 : p * 128 + 128]
                    ch = p * 2 + e
                    part[n, ch, :, 0:128] = (re * wr + im * wi).astype(BF)
                    part[n, ch, :, 128:256] = (im * wr - re * wi).astype(BF)
        for ch in range(4):
            sp = []
            for n in range(3):
                sp.append(jnp.dot(part[n, ch], t2_ref[...], preferred_element_type=F32))
            vr, vi = sp[0][:, :128], sp[0][:, 128:]
            gr, gi = sp[1][:, :128], sp[1][:, 128:]
            fr, fi = sp[2][:, :128], sp[2][:, 128:]
            prods = (
                (vr * fr - vi * fi, vr * fi + vi * fr),
                (fr * gr + fi * gi, fr * gi - fi * gr),
                (vr * gr + vi * gi, vr * gi - vi * gr),
            )
            for n in range(3):
                qq = jnp.concatenate([prods[n][0].astype(BF), prods[n][1].astype(BF)], axis=1)
                three = jnp.dot(qq, t3_ref[...], preferred_element_type=F32)
                re, im = three[:, :128], three[:, 128:]
                p, e = ch // 2, ch % 2
                spec[n, e * 256 : e * 256 + 128, p * 128 : p * 128 + 128] = (
                    re * wr - im * wi
                ).astype(BF)
                spec[n, e * 256 + 128 : e * 256 + 256, p * 128 : p * 128 + 128] = (
                    im * wr + re * wi
                ).astype(BF)
        for n in range(3):
            four = jnp.dot(t4_ref[...], spec[n], preferred_element_type=F32)
            if n == 2:
                four = four * (1.0 / 128.0)
            for p in range(2):
                made[g, n, pair + p] = four[:, p * 128 : p * 128 + 128].astype(BF)

    lane = lax.broadcasted_iota(jnp.int32, (1, 128), 1)
    sub = lax.broadcasted_iota(jnp.int32, (8, 128), 0)

    def direct_sums(g):
        row = jnp.zeros((1, 128), F32)
        for p in range(pairs):
            terms = held[g, 0, p].astype(F32) * held[g, 1, p].astype(F32)
            folded = jnp.sum(terms.reshape(32, 8, 128), axis=0)
            for e in range(2):
                own = jnp.where(lax.rem(sub, 2) == e, folded, 0.0)
                total = jnp.sum(jnp.sum(own, axis=1, keepdims=True), axis=0, keepdims=True)
                row = row + jnp.where(lane == g * per + p * 2 + e, total, 0.0)
        sk_own[...] = sk_own[...] + row

    def send_sums():
        own = sk_own[...]
        sk_own[...] = jnp.where(my_c == 0, own, pltpu.roll(own, per * GROUPS, 1))
        pltpu.make_async_remote_copy(
            src_ref=sk_own,
            dst_ref=sk_near,
            send_sem=near_send,
            recv_sem=near_recv,
            device_id=at_offset(1, 0, 0, 0),
            device_id_type=MESH,
        ).start()
        pltpu.make_async_copy(sk_near, sk_near, near_recv).wait()
        sk_row[...] = sk_own[...] + sk_near[...]

    def pass_sums():
        chip = pl.ds(lax.div(me, 2), 1)
        pltpu.make_async_copy(sk_row, sk_all.at[chip, :], sk_recv).start()
        for offset in sorted(offsets, key=lambda f: hops(f) <= 2):
            if offset[0] == 0:
                pltpu.make_async_remote_copy(
                    src_ref=sk_row,
                    dst_ref=sk_all.at[chip, :],
                    send_sem=sk_send,
                    recv_sem=sk_recv,
                    device_id=at_offset(*offset),
                    device_id_type=MESH,
                ).start()

    def spread_sums():
        pltpu.make_async_copy(sk_all, sk_all, sk_recv).wait()
        rows = lax.broadcasted_iota(jnp.int32, (64, 128), 0)
        cols = lax.broadcasted_iota(jnp.int32, (64, 128), 1)
        mine = lax.div(cols, 16) == lax.rem(rows, 8)
        source = lax.broadcasted_iota(jnp.int32, (128, 128), 0)
        place = lax.broadcasted_iota(jnp.int32, (128, 128), 1)
        base = lax.rem(lax.div(place, per), 2) * (per * GROUPS) + lax.rem(place, per)
        for g in range(GROUPS):
            pick = (source == base + g * per).astype(F32)
            wide = jnp.dot(
                sk_all[...], pick, preferred_element_type=F32, precision=lax.Precision.HIGHEST
            )
            kept = jnp.where(mine, wide, 0.0)
            sk_ref[g * 8 : g * 8 + 8, :] = jnp.sum(kept.reshape(8, 8, 128), axis=1) * (
                1.0 / 128.0
            )

    outs = (lo_ref, qg_ref, kg_ref, vg_ref, fg_ref)

    def finish(g):
        pltpu.make_async_copy(back.at[g], back.at[g], out_recv.at[g]).wait()

        def block(b, carry):
            cols = block_cols(g, b)
            rows = pl.ds(pl.multiple_of(b * 128, 128), 128)
            views = back.reshape(GROUPS - 1, 3, width, 128)
            results = results_of(
                [views[g, n, rows, :] for n in range(3)],
                [ins[n, :, cols] for n in range(4)],
                gain_ref[pl.ds(g * (width // 128) + b, 1), :],
            )
            for n in range(5):
                outs[n][:, cols] = results[n]
            return carry

        lax.fori_loop(0, width // 128, block, 0)

    sk_own[...] = jnp.zeros_like(sk_own)
    prepare(0)
    pl.semaphore_wait(barrier, DEVICES - 1)
    send_in(0)

    def ahead(g, carry):
        prepare(g)
        send_in(g)
        return carry

    lax.fori_loop(1, GROUPS, ahead, 0)

    for n, (source, place) in enumerate(fixed):
        pltpu.make_async_copy(source, place, table_sem.at[n]).wait()

    def middle(g, carry):
        pltpu.make_async_copy(held.at[g], held.at[g], in_recv.at[g]).wait()

        def half(h, inside):
            transform(g, h)
            return inside

        direct_sums(g)

        @pl.when(g == GROUPS - 1)
        def _():
            send_sums()

        lax.fori_loop(0, pairs // 2, half, 0)

        @pl.when(g == GROUPS - 1)
        def _():
            pass_sums()

        @pl.when(g < GROUPS - 1)
        def _():
            send_out(g, back.at[g])

        @pl.when(g == GROUPS - 1)
        def _():
            send_out(g, final, far_first=True)

        return carry

    lax.fori_loop(0, GROUPS, middle, 0)

    def ending(g, carry):
        finish(g)
        return carry

    lax.fori_loop(0, GROUPS - 1, ending, 0)
    spread_sums()
    everyone = held.at[:, :, :, pl.ds(0, 2 * (DEVICES - 1)), :]
    pltpu.make_async_copy(everyone, everyone, in_send).wait()
    pltpu.make_async_copy(sk_near, sk_near, near_send).wait()
    sums = sk_all.at[pl.ds(0, DEVICES // 2 - 1), :]
    pltpu.make_async_copy(sums, sums, sk_send).wait()
    pltpu.make_async_copy(final, final, out_recv.at[GROUPS - 1]).wait()
    pltpu.make_async_copy(everyone, everyone, out_send).wait()


def results_of(sums, rows, gain):
    conv, corr = sums[0].T.astype(F32), sums[1].T.astype(F32)
    kk, vv, gg, qq = (r.astype(F32) for r in rows)
    product = (kk * vv).astype(BF).astype(F32)
    mixing = conv + gain * product
    carried = corr + gain * (gg * qq)
    return (
        (qq * mixing).astype(BF),
        (gg * mixing).astype(BF),
        (carried * vv).astype(BF),
        (carried * kk).astype(BF),
        sums[2].T,
    )


def deliver(*refs):
    early, (ins, final, gain_ref, sums) = refs[:5], refs[5:9]
    whole, sums_out = refs[9:14], refs[14]
    late, sem = refs[15], refs[16]
    channels = whole[0].shape[1]
    width = channels // GROUPS
    first = channels - width
    parts = 2
    step = width // parts
    copies = [
        pltpu.make_async_copy(early[n], whole[n].at[:, pl.ds(0, first)], sem.at[n])
        for n in range(5)
    ]
    copies.append(pltpu.make_async_copy(sums, sums_out, sem.at[5]))
    for copy in copies:
        copy.start()
    views = final.reshape(3, width, 128)
    for part in range(parts):

        def block(b, carry):
            at = pl.multiple_of(part * step + b * 128, 128)
            cols = pl.ds(first + at, 128)
            results = results_of(
                [views[n, pl.ds(at, 128), :] for n in range(3)],
                [ins[n, :, cols] for n in range(4)],
                gain_ref[pl.ds((first + part * step) // 128 + b, 1), :],
            )
            for n in range(5):
                late[n, :, pl.ds(at, 128)] = results[n]
            return carry

        lax.fori_loop(0, step // 128, block, 0)
        for n in range(5):
            copies.append(
                pltpu.make_async_copy(
                    late.at[n, :, pl.ds(part * step, step)],
                    whole[n].at[:, pl.ds(first + part * step, step)],
                    sem.at[6 + part * 5 + n],
                )
            )
            copies[-1].start()
    for copy in copies:
        copy.wait()


def body(query_rows, key_rows, value_rows, out_grad, filter_rows, skip_gain):
    tokens, channels = query_rows.shape
    length = tokens * DEVICES
    width = channels // GROUPS
    per = width // DEVICES
    tables = [jnp.asarray(t) for t in coefficient_tables(tokens, DEVICES, length)]
    rows = jax.ShapeDtypeStruct((tokens, channels), BF)
    anywhere = pl.BlockSpec(memory_space=pl.ANY)
    dma = pltpu.SemaphoreType.DMA
    sums = jax.ShapeDtypeStruct((channels // 128, 128), F32)
    early = jax.ShapeDtypeStruct((tokens, channels - width), BF)
    hbm = pl.BlockSpec(memory_space=pltpu.HBM)
    vmem = pl.BlockSpec(memory_space=pltpu.VMEM)
    handed = pl.pallas_call(
        kernel,
        out_shape=[early] * 5
        + [
            jax.ShapeDtypeStruct((5, tokens, channels), BF),
            jax.ShapeDtypeStruct((3, width // 2, 2, 128), BF),
            sums,
            sums,
        ],
        in_specs=[hbm] * 11,
        out_specs=[vmem] * 9,
        scratch_shapes=[
            *[pltpu.VMEM(t.shape, t.dtype) for t in tables],
            pltpu.VMEM((GROUPS, 3, width // 2, 2, 128), BF),
            pltpu.VMEM((GROUPS, 3, per // 2, 2 * DEVICES, 128), BF),
            pltpu.VMEM((GROUPS, 3, per // 2, 2 * DEVICES, 128), BF),
            pltpu.VMEM((GROUPS - 1, 3, width // 2, 2, 128), BF),
            pltpu.VMEM((3, 4, DEVICES, 256), BF),
            pltpu.VMEM((3, 4 * DEVICES, 256), BF),
            pltpu.VMEM((1, 128), F32),
            pltpu.VMEM((1, 128), F32),
            pltpu.VMEM((1, 128), F32),
            pltpu.VMEM((DEVICES // 2, 128), F32),
            dma((5, GROUPS)),
            dma((6,)),
            dma,
            dma((GROUPS,)),
            dma,
            dma((GROUPS,)),
            dma,
            dma,
            dma,
            dma,
        ],
        compiler_params=pltpu.CompilerParams(
            collective_id=0, has_side_effects=True, vmem_limit_bytes=VMEM_MAIN * 1024 * 1024
        ),
        name="hyena",
    )(
        *(
            pltpu.with_memory_space_constraint(a, pltpu.HBM)
            for a in (
                query_rows,
                key_rows,
                value_rows,
                out_grad,
                filter_rows,
                skip_gain.reshape(channels // 128, 128),
                *tables,
            )
        )
    )
    results = pl.pallas_call(
        deliver,
        out_shape=[rows] * 5 + [sums],
        in_specs=[anywhere] * 5 + [vmem] * 3 + [anywhere],
        out_specs=[hbm] * 6,
        scratch_shapes=[pltpu.VMEM((5, tokens, width), BF), dma((16,))],
        compiler_params=pltpu.CompilerParams(vmem_limit_bytes=VMEM_LAST * 1024 * 1024),
        name="deliver",
    )(*handed)
    return (*results[:5], results[5].reshape(channels))


def solution(mesh):
    rows = P(("outer", "inner"), None)
    return jax.shard_map(
        body,
        mesh=mesh,
        in_specs=(rows, rows, rows, rows, rows, P()),
        out_specs=(rows, rows, rows, rows, rows, P()),
        check_vma=False,
    )
```

```python
import functools
import math

import jax
import jax.numpy as jnp
import numpy as np
from jax import lax
from jax.experimental import pallas as pl
from jax.experimental.pallas import tpu as pltpu
from jax.sharding import PartitionSpec as P

MESH = pl.DeviceIdType.MESH
BF = jnp.bfloat16
F32 = jnp.float32
DEVICES = 128
GROUPS = 4
ORDER = 91
REACH = 3
VMEM_MAIN = 40
VMEM_LAST = 16


def coefficient_tables(tokens, devices, length):
    pos = np.arange(devices, dtype=np.float64)
    freq = np.arange(devices, dtype=np.float64) + 0.5
    step = np.arange(tokens, dtype=np.float64)
    one = 2.0 * np.pi * np.outer(freq, pos) / (2 * devices)
    first = np.zeros((2, 2, devices, devices, 2))
    for e in range(2):
        first[e, 0, :, :, e] = np.cos(one)
        first[e, 1, :, :, e] = -np.sin(one)
    first = first.reshape(4 * devices, 2 * devices)
    last = np.transpose(first) * (2.0 / (2 * length))
    two = 2.0 * np.pi * (np.outer(step, step) % tokens) / tokens
    c, s = np.cos(two), np.sin(two)
    forth = np.block([[c, -s], [s, c]])
    back = np.block([[c, s], [-s, c]])
    turn = 2.0 * np.pi * np.outer(freq, step) / (2 * length)
    as_bf = lambda t: np.asarray(t, np.float32).astype(jnp.bfloat16)
    return (
        as_bf(first),
        as_bf(forth),
        as_bf(back),
        as_bf(last),
        np.stack([np.cos(turn), np.sin(turn)]).astype(np.float32),
    )


def kernel(
    q_hbm,
    k_hbm,
    v_hbm,
    g_hbm,
    h_hbm,
    gain_hbm,
    t1_hbm,
    t2_hbm,
    t3_hbm,
    t4_hbm,
    tw_hbm,
    lo_ref,
    qg_ref,
    kg_ref,
    vg_ref,
    fg_ref,
    ins,
    final,
    gain_ref,
    sk_ref,
    t1_ref,
    t2_ref,
    t3_ref,
    t4_ref,
    tw_ref,
    packed,
    held,
    made,
    back,
    part,
    spec,
    sk_own,
    sk_near,
    sk_row,
    sk_all,
    load_sem,
    table_sem,
    in_send,
    in_recv,
    out_send,
    out_recv,
    sk_send,
    sk_recv,
    near_send,
    near_recv,
    gate,
):
    tokens, channels = q_hbm.shape
    width = channels // GROUPS
    per = width // DEVICES
    pairs = per // 2
    outer = lax.axis_index("outer")
    inner = lax.axis_index("inner")
    me = outer * 16 + inner
    my_y, my_zh = lax.rem(outer, 4), lax.div(outer, 4)
    my_c, my_x, my_zl = lax.rem(inner, 2), lax.rem(lax.div(inner, 2), 4), lax.div(inner, 8)
    my_z = my_zh * 2 + my_zl

    def target(k):
        j = lax.rem(k * ORDER, DEVICES)
        c = lax.rem(my_c + j, 2)
        x = lax.rem(my_x + lax.div(j, 2), 4)
        y = lax.rem(my_y + lax.div(j, 8), 4)
        z = lax.rem(my_z + lax.div(j, 32), 4)
        return lax.div(z, 2) * 4 + y, lax.rem(z, 2) * 8 + x * 2 + c

    barrier = pltpu.get_barrier_semaphore()
    o_z = [lax.div(lax.rem(my_z + d, 4), 2) * 4 for d in range(4)]
    i_z = [lax.rem(lax.rem(my_z + d, 4), 2) * 8 for d in range(4)]
    o_y = [lax.rem(my_y + d, 4) for d in range(4)]
    i_x = [lax.rem(my_x + d, 4) * 2 for d in range(4)]
    i_c = [my_c, 1 - my_c]

    def at_offset(c, x, y, z):
        return o_z[z] + o_y[y], i_z[z] + i_x[x] + i_c[c]

    offsets = [
        (j % 2, j // 2 % 4, j // 8 % 4, j // 32)
        for j in (k * ORDER % DEVICES for k in range(1, DEVICES))
    ]

    def hops(offset):
        return sum(min(d, 4 - d) for d in offset[1:])

    chips = sorted(
        (f for f in offsets if f[0] == 0), key=lambda f: (hops(f) > REACH, -hops(f))
    )
    near_count = 2 * sum(hops(f) <= REACH for f in chips) + 1
    far_count = 2 * sum(hops(f) > REACH for f in chips) + 1
    partner = at_offset(1, 0, 0, 0)

    def greet():
        pl.semaphore_signal(barrier, inc=1, device_id=partner, device_id_type=MESH)
        for _, x, y, z in chips:
            core = 0 if hops((0, x, y, z)) <= REACH else 1
            pl.semaphore_signal(
                barrier,
                inc=1,
                device_id=(o_z[z] + o_y[y], i_z[z] + i_x[x] + core),
                device_id_type=MESH,
            )

    def entered(core, count):
        @pl.when(my_c == core)
        def _():
            pl.semaphore_wait(barrier, count)
            pl.semaphore_signal(gate, inc=1, device_id=partner, device_id_type=MESH)

        @pl.when(my_c != core)
        def _():
            pl.semaphore_wait(gate, 1)

    hbm_in = (k_hbm, v_hbm, g_hbm, q_hbm, h_hbm)
    K, V, G, Q, H = range(5)

    def load(n, g):
        cols = pl.ds(pl.multiple_of(g * width, width), width)
        return pltpu.make_async_copy(hbm_in[n].at[:, cols], ins.at[n, :, cols], load_sem.at[n, g])

    for n in range(5):
        load(n, 0).start()
    greet()
    for g in range(1, GROUPS):
        for n in range(5):
            load(n, g).start()
    fixed = (
        (t1_hbm, t1_ref),
        (t2_hbm, t2_ref),
        (t3_hbm, t3_ref),
        (t4_hbm, t4_ref),
        (tw_hbm, tw_ref),
        (gain_hbm, gain_ref),
    )
    for n, (source, place) in enumerate(fixed):
        pltpu.make_async_copy(source, place, table_sem.at[n]).start()

    def block_cols(g, b):
        return pl.ds(pl.multiple_of(g * width + b * 128, 128), 128)

    def prepare(g):
        for n in range(5):
            load(n, g).wait()

        def block(b, carry):
            cols = block_cols(g, b)
            rows = pl.ds(pl.multiple_of(b * 128, 128), 128)
            product = ins[K, :, cols].astype(F32) * ins[V, :, cols].astype(F32)
            gate = ins[G, :, cols].astype(F32) * ins[Q, :, cols].astype(F32)
            packed.reshape(GROUPS, 3, width, 128)[g, 0, rows, :] = product.astype(BF).T
            packed.reshape(GROUPS, 3, width, 128)[g, 1, rows, :] = gate.astype(BF).T
            packed.reshape(GROUPS, 3, width, 128)[g, 2, rows, :] = ins[H, :, cols].T
            return carry

        lax.fori_loop(0, width // 128, block, 0)

    def send_in(g, first=False):
        def to(o, i):
            pltpu.make_async_remote_copy(
                src_ref=packed.at[g, :, pl.ds((o * 16 + i) * pairs, pairs)],
                dst_ref=held.at[g, :, :, pl.ds(me * 2, 2), :],
                send_sem=in_send,
                recv_sem=in_recv.at[g],
                device_id=(o, i),
                device_id_type=MESH,
            ).start()

        def one(k, carry):
            to(*target(k))
            return carry

        pltpu.make_async_copy(
            packed.at[g, :, pl.ds(me * pairs, pairs)],
            held.at[g, :, :, pl.ds(me * 2, 2), :],
            in_recv.at[g],
        ).start()
        if first:
            entered(0, near_count)
            for offset in offsets:
                if hops(offset) <= REACH:
                    to(*at_offset(*offset))
            entered(1, far_count)
            for offset in offsets:
                if hops(offset) > REACH:
                    to(*at_offset(*offset))
        else:
            lax.fori_loop(1, DEVICES, one, 0)

    def send_out(g, place, far_first=False):
        def to(o, i):
            pltpu.make_async_remote_copy(
                src_ref=made.at[g, :, :, pl.ds((o * 16 + i) * 2, 2), :],
                dst_ref=place.at[:, pl.ds(me * pairs, pairs)],
                send_sem=out_send,
                recv_sem=out_recv.at[g],
                device_id=(o, i),
                device_id_type=MESH,
            ).start()

        def one(k, carry):
            to(*target(k))
            return carry

        pltpu.make_async_copy(
            made.at[g, :, :, pl.ds(me * 2, 2), :],
            place.at[:, pl.ds(me * pairs, pairs)],
            out_recv.at[g],
        ).start()
        if far_first:
            for offset in sorted(offsets, key=lambda f: hops(f) <= 2):
                to(*at_offset(*offset))
        else:
            lax.fori_loop(1, DEVICES, one, 0)

    def transform(g, h):
        wr, wi = tw_ref[0], tw_ref[1]
        pair = h * 2
        for n in range(3):
            rhs = jnp.concatenate([held[g, n, pair], held[g, n, pair + 1]], axis=1)
            one = jnp.dot(t1_ref[...], rhs, preferred_element_type=F32)
            for e in range(2):
                for p in range(2):
                    re = one[e * 256 : e * 256 + 128, p * 128 : p * 128 + 128]
                    im = one[e * 256 + 128 : e * 256 + 256, p * 128 : p * 128 + 128]
                    ch = p * 2 + e
                    part[n, ch, :, 0:128] = (re * wr + im * wi).astype(BF)
                    part[n, ch, :, 128:256] = (im * wr - re * wi).astype(BF)
        for ch in range(4):
            sp = []
            for n in range(3):
                sp.append(jnp.dot(part[n, ch], t2_ref[...], preferred_element_type=F32))
            vr, vi = sp[0][:, :128], sp[0][:, 128:]
            gr, gi = sp[1][:, :128], sp[1][:, 128:]
            fr, fi = sp[2][:, :128], sp[2][:, 128:]
            prods = (
                (vr * fr - vi * fi, vr * fi + vi * fr),
                (fr * gr + fi * gi, fr * gi - fi * gr),
                (vr * gr + vi * gi, vr * gi - vi * gr),
            )
            for n in range(3):
                qq = jnp.concatenate([prods[n][0].astype(BF), prods[n][1].astype(BF)], axis=1)
                three = jnp.dot(qq, t3_ref[...], preferred_element_type=F32)
                re, im = three[:, :128], three[:, 128:]
                p, e = ch // 2, ch % 2
                spec[n, e * 256 : e * 256 + 128, p * 128 : p * 128 + 128] = (
                    re * wr - im * wi
                ).astype(BF)
                spec[n, e * 256 + 128 : e * 256 + 256, p * 128 : p * 128 + 128] = (
                    im * wr + re * wi
                ).astype(BF)
        for n in range(3):
            four = jnp.dot(t4_ref[...], spec[n], preferred_element_type=F32)
            if n == 2:
                four = four * (1.0 / 128.0)
            for p in range(2):
                made[g, n, pair + p] = four[:, p * 128 : p * 128 + 128].astype(BF)

    lane = lax.broadcasted_iota(jnp.int32, (1, 128), 1)
    sub = lax.broadcasted_iota(jnp.int32, (8, 128), 0)

    def direct_sums(g):
        row = jnp.zeros((1, 128), F32)
        for p in range(pairs):
            terms = held[g, 0, p].astype(F32) * held[g, 1, p].astype(F32)
            folded = jnp.sum(terms.reshape(32, 8, 128), axis=0)
            for e in range(2):
                own = jnp.where(lax.rem(sub, 2) == e, folded, 0.0)
                total = jnp.sum(jnp.sum(own, axis=1, keepdims=True), axis=0, keepdims=True)
                row = row + jnp.where(lane == g * per + p * 2 + e, total, 0.0)
        sk_own[...] = sk_own[...] + row

    def send_sums():
        own = sk_own[...]
        sk_own[...] = jnp.where(my_c == 0, own, pltpu.roll(own, per * GROUPS, 1))
        pltpu.make_async_remote_copy(
            src_ref=sk_own,
            dst_ref=sk_near,
            send_sem=near_send,
            recv_sem=near_recv,
            device_id=partner,
            device_id_type=MESH,
        ).start()
        pltpu.make_async_copy(sk_near, sk_near, near_recv).wait()
        sk_row[...] = sk_own[...] + sk_near[...]

    def pass_sums():
        chip = pl.ds(lax.div(me, 2), 1)
        pltpu.make_async_copy(sk_row, sk_all.at[chip, :], sk_recv).start()
        for offset in sorted(offsets, key=lambda f: hops(f) <= 2):
            if offset[0] == 0:
                pltpu.make_async_remote_copy(
                    src_ref=sk_row,
                    dst_ref=sk_all.at[chip, :],
                    send_sem=sk_send,
                    recv_sem=sk_recv,
                    device_id=at_offset(*offset),
                    device_id_type=MESH,
                ).start()

    def spread_sums():
        pltpu.make_async_copy(sk_all, sk_all, sk_recv).wait()
        rows = lax.broadcasted_iota(jnp.int32, (64, 128), 0)
        cols = lax.broadcasted_iota(jnp.int32, (64, 128), 1)
        mine = lax.div(cols, 16) == lax.rem(rows, 8)
        source = lax.broadcasted_iota(jnp.int32, (128, 128), 0)
        place = lax.broadcasted_iota(jnp.int32, (128, 128), 1)
        base = lax.rem(lax.div(place, per), 2) * (per * GROUPS) + lax.rem(place, per)
        for g in range(GROUPS):
            pick = (source == base + g * per).astype(F32)
            wide = jnp.dot(
                sk_all[...], pick, preferred_element_type=F32, precision=lax.Precision.HIGHEST
            )
            kept = jnp.where(mine, wide, 0.0)
            sk_ref[g * 8 : g * 8 + 8, :] = jnp.sum(kept.reshape(8, 8, 128), axis=1) * (
                1.0 / 128.0
            )

    outs = (lo_ref, qg_ref, kg_ref, vg_ref, fg_ref)

    def finish(g):
        pltpu.make_async_copy(back.at[g], back.at[g], out_recv.at[g]).wait()

        def block(b, carry):
            cols = block_cols(g, b)
            rows = pl.ds(pl.multiple_of(b * 128, 128), 128)
            views = back.reshape(GROUPS - 1, 3, width, 128)
            results = results_of(
                [views[g, n, rows, :] for n in range(3)],
                [ins[n, :, cols] for n in range(4)],
                gain_ref[pl.ds(g * (width // 128) + b, 1), :],
            )
            for n in range(5):
                outs[n][:, cols] = results[n]
            return carry

        lax.fori_loop(0, width // 128, block, 0)

    sk_own[...] = jnp.zeros_like(sk_own)
    prepare(0)
    send_in(0, first=True)

    def ahead(g, carry):
        prepare(g)
        send_in(g)
        return carry

    lax.fori_loop(1, GROUPS, ahead, 0)

    for n, (source, place) in enumerate(fixed):
        pltpu.make_async_copy(source, place, table_sem.at[n]).wait()

    def middle(g, carry):
        pltpu.make_async_copy(held.at[g], held.at[g], in_recv.at[g]).wait()

        def half(h, inside):
            transform(g, h)
            return inside

        direct_sums(g)

        @pl.when(g == GROUPS - 1)
        def _():
            send_sums()

        lax.fori_loop(0, pairs // 2, half, 0)

        @pl.when(g == GROUPS - 1)
        def _():
            pass_sums()

        @pl.when(g < GROUPS - 1)
        def _():
            send_out(g, back.at[g])

        @pl.when(g == GROUPS - 1)
        def _():
            send_out(g, final, far_first=True)

        return carry

    lax.fori_loop(0, GROUPS, middle, 0)

    def ending(g, carry):
        finish(g)
        return carry

    lax.fori_loop(0, GROUPS - 1, ending, 0)
    spread_sums()
    everyone = held.at[:, :, :, pl.ds(0, 2 * (DEVICES - 1)), :]
    pltpu.make_async_copy(everyone, everyone, in_send).wait()
    pltpu.make_async_copy(sk_near, sk_near, near_send).wait()
    sums = sk_all.at[pl.ds(0, DEVICES // 2 - 1), :]
    pltpu.make_async_copy(sums, sums, sk_send).wait()
    pltpu.make_async_copy(final, final, out_recv.at[GROUPS - 1]).wait()
    pltpu.make_async_copy(everyone, everyone, out_send).wait()


def results_of(sums, rows, gain):
    conv, corr = sums[0].T.astype(F32), sums[1].T.astype(F32)
    kk, vv, gg, qq = (r.astype(F32) for r in rows)
    product = (kk * vv).astype(BF).astype(F32)
    mixing = conv + gain * product
    carried = corr + gain * (gg * qq)
    return (
        (qq * mixing).astype(BF),
        (gg * mixing).astype(BF),
        (carried * vv).astype(BF),
        (carried * kk).astype(BF),
        sums[2].T,
    )


def deliver(*refs):
    early, (ins, final, gain_ref, sums) = refs[:5], refs[5:9]
    whole, sums_out = refs[9:14], refs[14]
    late, sem = refs[15], refs[16]
    channels = whole[0].shape[1]
    width = channels // GROUPS
    first = channels - width
    parts = 2
    step = width // parts
    copies = [
        pltpu.make_async_copy(early[n], whole[n].at[:, pl.ds(0, first)], sem.at[n])
        for n in range(5)
    ]
    copies.append(pltpu.make_async_copy(sums, sums_out, sem.at[5]))
    for copy in copies:
        copy.start()
    views = final.reshape(3, width, 128)
    for part in range(parts):

        def block(b, carry):
            at = pl.multiple_of(part * step + b * 128, 128)
            cols = pl.ds(first + at, 128)
            results = results_of(
                [views[n, pl.ds(at, 128), :] for n in range(3)],
                [ins[n, :, cols] for n in range(4)],
                gain_ref[pl.ds((first + part * step) // 128 + b, 1), :],
            )
            for n in range(5):
                late[n, :, pl.ds(at, 128)] = results[n]
            return carry

        lax.fori_loop(0, step // 128, block, 0)
        for n in range(5):
            copies.append(
                pltpu.make_async_copy(
                    late.at[n, :, pl.ds(part * step, step)],
                    whole[n].at[:, pl.ds(first + part * step, step)],
                    sem.at[6 + part * 5 + n],
                )
            )
            copies[-1].start()
    for copy in copies:
        copy.wait()


def body(query_rows, key_rows, value_rows, out_grad, filter_rows, skip_gain):
    tokens, channels = query_rows.shape
    length = tokens * DEVICES
    width = channels // GROUPS
    per = width // DEVICES
    tables = [jnp.asarray(t) for t in coefficient_tables(tokens, DEVICES, length)]
    rows = jax.ShapeDtypeStruct((tokens, channels), BF)
    anywhere = pl.BlockSpec(memory_space=pl.ANY)
    dma = pltpu.SemaphoreType.DMA
    sums = jax.ShapeDtypeStruct((channels // 128, 128), F32)
    early = jax.ShapeDtypeStruct((tokens, channels - width), BF)
    hbm = pl.BlockSpec(memory_space=pltpu.HBM)
    vmem = pl.BlockSpec(memory_space=pltpu.VMEM)
    handed = pl.pallas_call(
        kernel,
        out_shape=[early] * 5
        + [
            jax.ShapeDtypeStruct((5, tokens, channels), BF),
            jax.ShapeDtypeStruct((3, width // 2, 2, 128), BF),
            sums,
            sums,
        ],
        in_specs=[hbm] * 11,
        out_specs=[vmem] * 9,
        scratch_shapes=[
            *[pltpu.VMEM(t.shape, t.dtype) for t in tables],
            pltpu.VMEM((GROUPS, 3, width // 2, 2, 128), BF),
            pltpu.VMEM((GROUPS, 3, per // 2, 2 * DEVICES, 128), BF),
            pltpu.VMEM((GROUPS, 3, per // 2, 2 * DEVICES, 128), BF),
            pltpu.VMEM((GROUPS - 1, 3, width // 2, 2, 128), BF),
            pltpu.VMEM((3, 4, DEVICES, 256), BF),
            pltpu.VMEM((3, 4 * DEVICES, 256), BF),
            pltpu.VMEM((1, 128), F32),
            pltpu.VMEM((1, 128), F32),
            pltpu.VMEM((1, 128), F32),
            pltpu.VMEM((DEVICES // 2, 128), F32),
            dma((5, GROUPS)),
            dma((6,)),
            dma,
            dma((GROUPS,)),
            dma,
            dma((GROUPS,)),
            dma,
            dma,
            dma,
            dma,
            pltpu.SemaphoreType.REGULAR,
        ],
        compiler_params=pltpu.CompilerParams(
            collective_id=0, has_side_effects=True, vmem_limit_bytes=VMEM_MAIN * 1024 * 1024
        ),
        name="hyena",
    )(
        *(
            pltpu.with_memory_space_constraint(a, pltpu.HBM)
            for a in (
                query_rows,
                key_rows,
                value_rows,
                out_grad,
                filter_rows,
                skip_gain.reshape(channels // 128, 128),
                *tables,
            )
        )
    )
    results = pl.pallas_call(
        deliver,
        out_shape=[rows] * 5 + [sums],
        in_specs=[anywhere] * 5 + [vmem] * 3 + [anywhere],
        out_specs=[hbm] * 6,
        scratch_shapes=[pltpu.VMEM((5, tokens, width), BF), dma((16,))],
        compiler_params=pltpu.CompilerParams(vmem_limit_bytes=VMEM_LAST * 1024 * 1024),
        name="deliver",
    )(*handed)
    return (*results[:5], results[5].reshape(channels))


def solution(mesh):
    rows = P(("outer", "inner"), None)
    return jax.shard_map(
        body,
        mesh=mesh,
        in_specs=(rows, rows, rows, rows, rows, P()),
        out_specs=(rows, rows, rows, rows, rows, P()),
        check_vma=False,
    )
```

```python
import functools
import math

import jax
import jax.numpy as jnp
import numpy as np
from jax import lax
from jax.experimental import pallas as pl
from jax.experimental.pallas import tpu as pltpu
from jax.sharding import PartitionSpec as P

MESH = pl.DeviceIdType.MESH
BF = jnp.bfloat16
F32 = jnp.float32
DEVICES = 128
GROUPS = 4
ORDER = 91
REACH = 2
VMEM_MAIN = 40
VMEM_LAST = 16


def coefficient_tables(tokens, devices, length):
    pos = np.arange(devices, dtype=np.float64)
    freq = np.arange(devices, dtype=np.float64) + 0.5
    step = np.arange(tokens, dtype=np.float64)
    one = 2.0 * np.pi * np.outer(freq, pos) / (2 * devices)
    first = np.zeros((2, 2, devices, devices, 2))
    for e in range(2):
        first[e, 0, :, :, e] = np.cos(one)
        first[e, 1, :, :, e] = -np.sin(one)
    first = first.reshape(4 * devices, 2 * devices)
    last = np.transpose(first) * (2.0 / (2 * length))
    two = 2.0 * np.pi * (np.outer(step, step) % tokens) / tokens
    c, s = np.cos(two), np.sin(two)
    forth = np.block([[c, -s], [s, c]])
    back = np.block([[c, s], [-s, c]])
    turn = 2.0 * np.pi * np.outer(freq, step) / (2 * length)
    as_bf = lambda t: np.asarray(t, np.float32).astype(jnp.bfloat16)
    return (
        as_bf(first),
        as_bf(forth),
        as_bf(back),
        as_bf(last),
        np.stack([np.cos(turn), np.sin(turn)]).astype(np.float32),
    )


def kernel(
    q_hbm,
    k_hbm,
    v_hbm,
    g_hbm,
    h_hbm,
    gain_hbm,
    t1_hbm,
    t2_hbm,
    t3_hbm,
    t4_hbm,
    tw_hbm,
    lo_ref,
    qg_ref,
    kg_ref,
    vg_ref,
    fg_ref,
    ins,
    final,
    gain_ref,
    sk_ref,
    t1_ref,
    t2_ref,
    t3_ref,
    t4_ref,
    tw_ref,
    packed,
    held,
    made,
    back,
    part,
    spec,
    sk_own,
    sk_near,
    sk_row,
    sk_all,
    load_sem,
    table_sem,
    in_send,
    in_recv,
    out_send,
    out_recv,
    sk_send,
    sk_recv,
    near_send,
    near_recv,
    gate,
):
    tokens, channels = q_hbm.shape
    width = channels // GROUPS
    per = width // DEVICES
    pairs = per // 2
    outer = lax.axis_index("outer")
    inner = lax.axis_index("inner")
    me = outer * 16 + inner
    my_y, my_zh = lax.rem(outer, 4), lax.div(outer, 4)
    my_c, my_x, my_zl = lax.rem(inner, 2), lax.rem(lax.div(inner, 2), 4), lax.div(inner, 8)
    my_z = my_zh * 2 + my_zl

    def target(k):
        j = lax.rem(k * ORDER, DEVICES)
        c = lax.rem(my_c + j, 2)
        x = lax.rem(my_x + lax.div(j, 2), 4)
        y = lax.rem(my_y + lax.div(j, 8), 4)
        z = lax.rem(my_z + lax.div(j, 32), 4)
        return lax.div(z, 2) * 4 + y, lax.rem(z, 2) * 8 + x * 2 + c

    barrier = pltpu.get_barrier_semaphore()
    o_z = [lax.div(lax.rem(my_z + d, 4), 2) * 4 for d in range(4)]
    i_z = [lax.rem(lax.rem(my_z + d, 4), 2) * 8 for d in range(4)]
    o_y = [lax.rem(my_y + d, 4) for d in range(4)]
    i_x = [lax.rem(my_x + d, 4) * 2 for d in range(4)]
    i_c = [my_c, 1 - my_c]

    def at_offset(c, x, y, z):
        return o_z[z] + o_y[y], i_z[z] + i_x[x] + i_c[c]

    offsets = [
        (j % 2, j // 2 % 4, j // 8 % 4, j // 32)
        for j in (k * ORDER % DEVICES for k in range(1, DEVICES))
    ]

    def hops(offset):
        return sum(min(d, 4 - d) for d in offset[1:])

    chips = sorted(
        (f for f in offsets if f[0] == 0), key=lambda f: (hops(f) > REACH, -hops(f))
    )
    near_count = 2 * sum(hops(f) <= REACH for f in chips) + 1
    far_count = 2 * sum(hops(f) > REACH for f in chips) + 1
    partner = at_offset(1, 0, 0, 0)

    def greet():
        pl.semaphore_signal(barrier, inc=1, device_id=partner, device_id_type=MESH)
        for _, x, y, z in chips:
            core = 0 if hops((0, x, y, z)) <= REACH else 1
            pl.semaphore_signal(
                barrier,
                inc=1,
                device_id=(o_z[z] + o_y[y], i_z[z] + i_x[x] + core),
                device_id_type=MESH,
            )

    def entered(core, count):
        @pl.when(my_c == core)
        def _():
            pl.semaphore_wait(barrier, count)
            pl.semaphore_signal(gate, inc=1, device_id=partner, device_id_type=MESH)

        @pl.when(my_c != core)
        def _():
            pl.semaphore_wait(gate, 1)

    hbm_in = (k_hbm, v_hbm, g_hbm, q_hbm, h_hbm)
    K, V, G, Q, H = range(5)

    def load(n, g):
        cols = pl.ds(pl.multiple_of(g * width, width), width)
        return pltpu.make_async_copy(hbm_in[n].at[:, cols], ins.at[n, :, cols], load_sem.at[n, g])

    for n in range(5):
        load(n, 0).start()
    greet()
    for g in range(1, GROUPS):
        for n in range(5):
            load(n, g).start()
    fixed = (
        (t1_hbm, t1_ref),
        (t2_hbm, t2_ref),
        (t3_hbm, t3_ref),
        (t4_hbm, t4_ref),
        (tw_hbm, tw_ref),
        (gain_hbm, gain_ref),
    )
    for n, (source, place) in enumerate(fixed):
        pltpu.make_async_copy(source, place, table_sem.at[n]).start()

    def block_cols(g, b):
        return pl.ds(pl.multiple_of(g * width + b * 128, 128), 128)

    def prepare(g):
        for n in range(5):
            load(n, g).wait()

        def block(b, carry):
            cols = block_cols(g, b)
            rows = pl.ds(pl.multiple_of(b * 128, 128), 128)
            product = ins[K, :, cols].astype(F32) * ins[V, :, cols].astype(F32)
            gate = ins[G, :, cols].astype(F32) * ins[Q, :, cols].astype(F32)
            packed.reshape(GROUPS, 3, width, 128)[g, 0, rows, :] = product.astype(BF).T
            packed.reshape(GROUPS, 3, width, 128)[g, 1, rows, :] = gate.astype(BF).T
            packed.reshape(GROUPS, 3, width, 128)[g, 2, rows, :] = ins[H, :, cols].T
            return carry

        lax.fori_loop(0, width // 128, block, 0)

    def send_in(g, first=False):
        def to(o, i):
            pltpu.make_async_remote_copy(
                src_ref=packed.at[g, :, pl.ds((o * 16 + i) * pairs, pairs)],
                dst_ref=held.at[g, :, :, pl.ds(me * 2, 2), :],
                send_sem=in_send,
                recv_sem=in_recv.at[g],
                device_id=(o, i),
                device_id_type=MESH,
            ).start()

        def one(k, carry):
            to(*target(k))
            return carry

        pltpu.make_async_copy(
            packed.at[g, :, pl.ds(me * pairs, pairs)],
            held.at[g, :, :, pl.ds(me * 2, 2), :],
            in_recv.at[g],
        ).start()
        if first:
            entered(0, near_count)
            for offset in offsets:
                if hops(offset) <= REACH:
                    to(*at_offset(*offset))
            entered(1, far_count)
            for offset in offsets:
                if hops(offset) > REACH:
                    to(*at_offset(*offset))
        else:
            lax.fori_loop(1, DEVICES, one, 0)

    def send_out(g, place, far_first=False):
        def to(o, i):
            pltpu.make_async_remote_copy(
                src_ref=made.at[g, :, :, pl.ds((o * 16 + i) * 2, 2), :],
                dst_ref=place.at[:, pl.ds(me * pairs, pairs)],
                send_sem=out_send,
                recv_sem=out_recv.at[g],
                device_id=(o, i),
                device_id_type=MESH,
            ).start()

        def one(k, carry):
            to(*target(k))
            return carry

        pltpu.make_async_copy(
            made.at[g, :, :, pl.ds(me * 2, 2), :],
            place.at[:, pl.ds(me * pairs, pairs)],
            out_recv.at[g],
        ).start()
        if far_first:
            for offset in sorted(offsets, key=lambda f: hops(f) <= 2):
                to(*at_offset(*offset))
        else:
            lax.fori_loop(1, DEVICES, one, 0)

    def transform(g, h):
        wr, wi = tw_ref[0], tw_ref[1]
        pair = h * 2
        for n in range(3):
            rhs = jnp.concatenate([held[g, n, pair], held[g, n, pair + 1]], axis=1)
            one = jnp.dot(t1_ref[...], rhs, preferred_element_type=F32)
            for e in range(2):
                for p in range(2):
                    re = one[e * 256 : e * 256 + 128, p * 128 : p * 128 + 128]
                    im = one[e * 256 + 128 : e * 256 + 256, p * 128 : p * 128 + 128]
                    ch = p * 2 + e
                    part[n, ch, :, 0:128] = (re * wr + im * wi).astype(BF)
                    part[n, ch, :, 128:256] = (im * wr - re * wi).astype(BF)
        for ch in range(4):
            sp = []
            for n in range(3):
                sp.append(jnp.dot(part[n, ch], t2_ref[...], preferred_element_type=F32))
            vr, vi = sp[0][:, :128], sp[0][:, 128:]
            gr, gi = sp[1][:, :128], sp[1][:, 128:]
            fr, fi = sp[2][:, :128], sp[2][:, 128:]
            prods = (
                (vr * fr - vi * fi, vr * fi + vi * fr),
                (fr * gr + fi * gi, fr * gi - fi * gr),
                (vr * gr + vi * gi, vr * gi - vi * gr),
            )
            for n in range(3):
                qq = jnp.concatenate([prods[n][0].astype(BF), prods[n][1].astype(BF)], axis=1)
                three = jnp.dot(qq, t3_ref[...], preferred_element_type=F32)
                re, im = three[:, :128], three[:, 128:]
                p, e = ch // 2, ch % 2
                spec[n, e * 256 : e * 256 + 128, p * 128 : p * 128 + 128] = (
                    re * wr - im * wi
                ).astype(BF)
                spec[n, e * 256 + 128 : e * 256 + 256, p * 128 : p * 128 + 128] = (
                    im * wr + re * wi
                ).astype(BF)
        for n in range(3):
            four = jnp.dot(t4_ref[...], spec[n], preferred_element_type=F32)
            if n == 2:
                four = four * (1.0 / 128.0)
            for p in range(2):
                made[g, n, pair + p] = four[:, p * 128 : p * 128 + 128].astype(BF)

    lane = lax.broadcasted_iota(jnp.int32, (1, 128), 1)
    sub = lax.broadcasted_iota(jnp.int32, (8, 128), 0)

    def direct_sums(g):
        row = jnp.zeros((1, 128), F32)
        for p in range(pairs):
            terms = held[g, 0, p].astype(F32) * held[g, 1, p].astype(F32)
            folded = jnp.sum(terms.reshape(32, 8, 128), axis=0)
            for e in range(2):
                own = jnp.where(lax.rem(sub, 2) == e, folded, 0.0)
                total = jnp.sum(jnp.sum(own, axis=1, keepdims=True), axis=0, keepdims=True)
                row = row + jnp.where(lane == g * per + p * 2 + e, total, 0.0)
        sk_own[...] = sk_own[...] + row

    def send_sums():
        own = sk_own[...]
        sk_own[...] = jnp.where(my_c == 0, own, pltpu.roll(own, per * GROUPS, 1))
        pltpu.make_async_remote_copy(
            src_ref=sk_own,
            dst_ref=sk_near,
            send_sem=near_send,
            recv_sem=near_recv,
            device_id=partner,
            device_id_type=MESH,
        ).start()
        pltpu.make_async_copy(sk_near, sk_near, near_recv).wait()
        sk_row[...] = sk_own[...] + sk_near[...]

    def pass_sums():
        chip = pl.ds(lax.div(me, 2), 1)
        pltpu.make_async_copy(sk_row, sk_all.at[chip, :], sk_recv).start()
        for offset in sorted(offsets, key=lambda f: hops(f) <= 2):
            if offset[0] == 0:
                pltpu.make_async_remote_copy(
                    src_ref=sk_row,
                    dst_ref=sk_all.at[chip, :],
                    send_sem=sk_send,
                    recv_sem=sk_recv,
                    device_id=at_offset(*offset),
                    device_id_type=MESH,
                ).start()

    def spread_sums():
        pltpu.make_async_copy(sk_all, sk_all, sk_recv).wait()
        rows = lax.broadcasted_iota(jnp.int32, (64, 128), 0)
        cols = lax.broadcasted_iota(jnp.int32, (64, 128), 1)
        mine = lax.div(cols, 16) == lax.rem(rows, 8)
        source = lax.broadcasted_iota(jnp.int32, (128, 128), 0)
        place = lax.broadcasted_iota(jnp.int32, (128, 128), 1)
        base = lax.rem(lax.div(place, per), 2) * (per * GROUPS) + lax.rem(place, per)
        for g in range(GROUPS):
            pick = (source == base + g * per).astype(F32)
            wide = jnp.dot(
                sk_all[...], pick, preferred_element_type=F32, precision=lax.Precision.HIGHEST
            )
            kept = jnp.where(mine, wide, 0.0)
            sk_ref[g * 8 : g * 8 + 8, :] = jnp.sum(kept.reshape(8, 8, 128), axis=1) * (
                1.0 / 128.0
            )

    outs = (lo_ref, qg_ref, kg_ref, vg_ref, fg_ref)

    def finish(g):
        pltpu.make_async_copy(back.at[g], back.at[g], out_recv.at[g]).wait()

        def block(b, carry):
            cols = block_cols(g, b)
            rows = pl.ds(pl.multiple_of(b * 128, 128), 128)
            views = back.reshape(GROUPS - 1, 3, width, 128)
            results = results_of(
                [views[g, n, rows, :] for n in range(3)],
                [ins[n, :, cols] for n in range(4)],
                gain_ref[pl.ds(g * (width // 128) + b, 1), :],
            )
            for n in range(5):
                outs[n][:, cols] = results[n]
            return carry

        lax.fori_loop(0, width // 128, block, 0)

    sk_own[...] = jnp.zeros_like(sk_own)
    prepare(0)
    send_in(0, first=True)

    def ahead(g, carry):
        prepare(g)
        send_in(g)
        return carry

    lax.fori_loop(1, GROUPS, ahead, 0)

    for n, (source, place) in enumerate(fixed):
        pltpu.make_async_copy(source, place, table_sem.at[n]).wait()

    def middle(g, carry):
        pltpu.make_async_copy(held.at[g], held.at[g], in_recv.at[g]).wait()

        def half(h, inside):
            transform(g, h)
            return inside

        direct_sums(g)

        @pl.when(g == GROUPS - 1)
        def _():
            send_sums()

        lax.fori_loop(0, pairs // 2, half, 0)

        @pl.when(g == GROUPS - 1)
        def _():
            pass_sums()

        @pl.when(g < GROUPS - 1)
        def _():
            send_out(g, back.at[g])

        @pl.when(g == GROUPS - 1)
        def _():
            send_out(g, final, far_first=True)

        return carry

    lax.fori_loop(0, GROUPS, middle, 0)

    def ending(g, carry):
        finish(g)
        return carry

    lax.fori_loop(0, GROUPS - 1, ending, 0)
    spread_sums()
    everyone = held.at[:, :, :, pl.ds(0, 2 * (DEVICES - 1)), :]
    pltpu.make_async_copy(everyone, everyone, in_send).wait()
    pltpu.make_async_copy(sk_near, sk_near, near_send).wait()
    sums = sk_all.at[pl.ds(0, DEVICES // 2 - 1), :]
    pltpu.make_async_copy(sums, sums, sk_send).wait()
    pltpu.make_async_copy(final, final, out_recv.at[GROUPS - 1]).wait()
    pltpu.make_async_copy(everyone, everyone, out_send).wait()


def results_of(sums, rows, gain):
    conv, corr = sums[0].T.astype(F32), sums[1].T.astype(F32)
    kk, vv, gg, qq = (r.astype(F32) for r in rows)
    product = (kk * vv).astype(BF).astype(F32)
    mixing = conv + gain * product
    carried = corr + gain * (gg * qq)
    return (
        (qq * mixing).astype(BF),
        (gg * mixing).astype(BF),
        (carried * vv).astype(BF),
        (carried * kk).astype(BF),
        sums[2].T,
    )


def deliver(*refs):
    early, (ins, final, gain_ref, sums) = refs[:5], refs[5:9]
    whole, sums_out = refs[9:14], refs[14]
    late, sem = refs[15], refs[16]
    channels = whole[0].shape[1]
    width = channels // GROUPS
    first = channels - width
    parts = 2
    step = width // parts
    copies = [
        pltpu.make_async_copy(early[n], whole[n].at[:, pl.ds(0, first)], sem.at[n])
        for n in range(5)
    ]
    copies.append(pltpu.make_async_copy(sums, sums_out, sem.at[5]))
    for copy in copies:
        copy.start()
    views = final.reshape(3, width, 128)
    for part in range(parts):

        def block(b, carry):
            at = pl.multiple_of(part * step + b * 128, 128)
            cols = pl.ds(first + at, 128)
            results = results_of(
                [views[n, pl.ds(at, 128), :] for n in range(3)],
                [ins[n, :, cols] for n in range(4)],
                gain_ref[pl.ds((first + part * step) // 128 + b, 1), :],
            )
            for n in range(5):
                late[n, :, pl.ds(at, 128)] = results[n]
            return carry

        lax.fori_loop(0, step // 128, block, 0)
        for n in range(5):
            copies.append(
                pltpu.make_async_copy(
                    late.at[n, :, pl.ds(part * step, step)],
                    whole[n].at[:, pl.ds(first + part * step, step)],
                    sem.at[6 + part * 5 + n],
                )
            )
            copies[-1].start()
    for copy in copies:
        copy.wait()


def body(query_rows, key_rows, value_rows, out_grad, filter_rows, skip_gain):
    tokens, channels = query_rows.shape
    length = tokens * DEVICES
    width = channels // GROUPS
    per = width // DEVICES
    tables = [jnp.asarray(t) for t in coefficient_tables(tokens, DEVICES, length)]
    rows = jax.ShapeDtypeStruct((tokens, channels), BF)
    anywhere = pl.BlockSpec(memory_space=pl.ANY)
    dma = pltpu.SemaphoreType.DMA
    sums = jax.ShapeDtypeStruct((channels // 128, 128), F32)
    early = jax.ShapeDtypeStruct((tokens, channels - width), BF)
    hbm = pl.BlockSpec(memory_space=pltpu.HBM)
    vmem = pl.BlockSpec(memory_space=pltpu.VMEM)
    handed = pl.pallas_call(
        kernel,
        out_shape=[early] * 5
        + [
            jax.ShapeDtypeStruct((5, tokens, channels), BF),
            jax.ShapeDtypeStruct((3, width // 2, 2, 128), BF),
            sums,
            sums,
        ],
        in_specs=[hbm] * 11,
        out_specs=[vmem] * 9,
        scratch_shapes=[
            *[pltpu.VMEM(t.shape, t.dtype) for t in tables],
            pltpu.VMEM((GROUPS, 3, width // 2, 2, 128), BF),
            pltpu.VMEM((GROUPS, 3, per // 2, 2 * DEVICES, 128), BF),
            pltpu.VMEM((GROUPS, 3, per // 2, 2 * DEVICES, 128), BF),
            pltpu.VMEM((GROUPS - 1, 3, width // 2, 2, 128), BF),
            pltpu.VMEM((3, 4, DEVICES, 256), BF),
            pltpu.VMEM((3, 4 * DEVICES, 256), BF),
            pltpu.VMEM((1, 128), F32),
            pltpu.VMEM((1, 128), F32),
            pltpu.VMEM((1, 128), F32),
            pltpu.VMEM((DEVICES // 2, 128), F32),
            dma((5, GROUPS)),
            dma((6,)),
            dma,
            dma((GROUPS,)),
            dma,
            dma((GROUPS,)),
            dma,
            dma,
            dma,
            dma,
            pltpu.SemaphoreType.REGULAR,
        ],
        compiler_params=pltpu.CompilerParams(
            collective_id=0, has_side_effects=True, vmem_limit_bytes=VMEM_MAIN * 1024 * 1024
        ),
        name="hyena",
    )(
        *(
            pltpu.with_memory_space_constraint(a, pltpu.HBM)
            for a in (
                query_rows,
                key_rows,
                value_rows,
                out_grad,
                filter_rows,
                skip_gain.reshape(channels // 128, 128),
                *tables,
            )
        )
    )
    results = pl.pallas_call(
        deliver,
        out_shape=[rows] * 5 + [sums],
        in_specs=[anywhere] * 5 + [vmem] * 3 + [anywhere],
        out_specs=[hbm] * 6,
        scratch_shapes=[pltpu.VMEM((5, tokens, width), BF), dma((16,))],
        compiler_params=pltpu.CompilerParams(vmem_limit_bytes=VMEM_LAST * 1024 * 1024),
        name="deliver",
    )(*handed)
    return (*results[:5], results[5].reshape(channels))


def solution(mesh):
    rows = P(("outer", "inner"), None)
    return jax.shard_map(
        body,
        mesh=mesh,
        in_specs=(rows, rows, rows, rows, rows, P()),
        out_specs=(rows, rows, rows, rows, rows, P()),
        check_vma=False,
    )
```

```python
import functools
import math

import jax
import jax.numpy as jnp
import numpy as np
from jax import lax
from jax.experimental import pallas as pl
from jax.experimental.pallas import tpu as pltpu
from jax.sharding import PartitionSpec as P

MESH = pl.DeviceIdType.MESH
BF = jnp.bfloat16
F32 = jnp.float32
DEVICES = 128
GROUPS = 4
ORDER = 91
REACH = 2
VMEM_MAIN = 40
VMEM_LAST = 16


def coefficient_tables(tokens, devices, length):
    pos = np.arange(devices, dtype=np.float64)
    freq = np.arange(devices, dtype=np.float64) + 0.5
    step = np.arange(tokens, dtype=np.float64)
    one = 2.0 * np.pi * np.outer(freq, pos) / (2 * devices)
    first = np.zeros((2, 2, devices, devices, 2))
    for e in range(2):
        first[e, 0, :, :, e] = np.cos(one)
        first[e, 1, :, :, e] = -np.sin(one)
    first = first.reshape(4 * devices, 2 * devices)
    last = np.transpose(first) * (2.0 / (2 * length))
    two = 2.0 * np.pi * (np.outer(step, step) % tokens) / tokens
    c, s = np.cos(two), np.sin(two)
    forth = np.block([[c, -s], [s, c]])
    back = np.block([[c, s], [-s, c]])
    turn = 2.0 * np.pi * np.outer(freq, step) / (2 * length)
    as_bf = lambda t: np.asarray(t, np.float32).astype(jnp.bfloat16)
    return (
        as_bf(first),
        as_bf(forth),
        as_bf(back),
        as_bf(last),
        np.stack([np.cos(turn), np.sin(turn)]).astype(np.float32),
    )


def kernel(
    q_hbm,
    k_hbm,
    v_hbm,
    g_hbm,
    h_hbm,
    gain_hbm,
    t1_hbm,
    t2_hbm,
    t3_hbm,
    t4_hbm,
    tw_hbm,
    lo_ref,
    qg_ref,
    kg_ref,
    vg_ref,
    fg_ref,
    ins,
    final,
    gain_ref,
    sk_ref,
    t1_ref,
    t2_ref,
    t3_ref,
    t4_ref,
    tw_ref,
    packed,
    held,
    made,
    back,
    part,
    spec,
    sk_own,
    sk_near,
    sk_row,
    sk_all,
    load_sem,
    table_sem,
    in_send,
    in_recv,
    out_send,
    out_recv,
    sk_send,
    sk_recv,
    near_send,
    near_recv,
    gate,
):
    tokens, channels = q_hbm.shape
    width = channels // GROUPS
    per = width // DEVICES
    pairs = per // 2
    outer = lax.axis_index("outer")
    inner = lax.axis_index("inner")
    me = outer * 16 + inner
    my_y, my_zh = lax.rem(outer, 4), lax.div(outer, 4)
    my_c, my_x, my_zl = lax.rem(inner, 2), lax.rem(lax.div(inner, 2), 4), lax.div(inner, 8)
    my_z = my_zh * 2 + my_zl

    def target(k):
        j = lax.rem(k * ORDER, DEVICES)
        c = lax.rem(my_c + j, 2)
        x = lax.rem(my_x + lax.div(j, 2), 4)
        y = lax.rem(my_y + lax.div(j, 8), 4)
        z = lax.rem(my_z + lax.div(j, 32), 4)
        return lax.div(z, 2) * 4 + y, lax.rem(z, 2) * 8 + x * 2 + c

    barrier = pltpu.get_barrier_semaphore()
    o_z = [lax.div(lax.rem(my_z + d, 4), 2) * 4 for d in range(4)]
    i_z = [lax.rem(lax.rem(my_z + d, 4), 2) * 8 for d in range(4)]
    o_y = [lax.rem(my_y + d, 4) for d in range(4)]
    i_x = [lax.rem(my_x + d, 4) * 2 for d in range(4)]
    i_c = [my_c, 1 - my_c]

    def at_offset(c, x, y, z):
        return o_z[z] + o_y[y], i_z[z] + i_x[x] + i_c[c]

    offsets = [
        (j % 2, j // 2 % 4, j // 8 % 4, j // 32)
        for j in (k * ORDER % DEVICES for k in range(1, DEVICES))
    ]

    def hops(offset):
        return sum(min(d, 4 - d) for d in offset[1:])

    chips = sorted(
        (f for f in offsets if f[0] == 0), key=lambda f: (hops(f) > REACH, -hops(f))
    )
    near_count = 2 * sum(hops(f) <= REACH for f in chips) + 1
    far_count = 2 * sum(hops(f) > REACH for f in chips) + 1
    partner = at_offset(1, 0, 0, 0)

    def greet():
        pl.semaphore_signal(barrier, inc=1, device_id=partner, device_id_type=MESH)
        for _, x, y, z in chips:
            core = 0 if hops((0, x, y, z)) <= REACH else 1
            pl.semaphore_signal(
                barrier,
                inc=1,
                device_id=(o_z[z] + o_y[y], i_z[z] + i_x[x] + core),
                device_id_type=MESH,
            )

    def entered(core, count):
        @pl.when(my_c == core)
        def _():
            pl.semaphore_wait(barrier, count)
            pl.semaphore_signal(gate, inc=1, device_id=partner, device_id_type=MESH)

        @pl.when(my_c != core)
        def _():
            pl.semaphore_wait(gate, 1)

    hbm_in = (k_hbm, v_hbm, g_hbm, q_hbm, h_hbm)
    K, V, G, Q, H = range(5)

    def load(n, g):
        cols = pl.ds(pl.multiple_of(g * width, width), width)
        return pltpu.make_async_copy(hbm_in[n].at[:, cols], ins.at[n, :, cols], load_sem.at[n, g])

    for n in range(5):
        load(n, 0).start()
    greet()
    for g in range(1, GROUPS):
        for n in range(5):
            load(n, g).start()
    fixed = (
        (t1_hbm, t1_ref),
        (t2_hbm, t2_ref),
        (t3_hbm, t3_ref),
        (t4_hbm, t4_ref),
        (tw_hbm, tw_ref),
        (gain_hbm, gain_ref),
    )
    for n, (source, place) in enumerate(fixed):
        pltpu.make_async_copy(source, place, table_sem.at[n]).start()

    def block_cols(g, b):
        return pl.ds(pl.multiple_of(g * width + b * 128, 128), 128)

    def prepare(g):
        for n in range(5):
            load(n, g).wait()

        def block(b, carry):
            cols = block_cols(g, b)
            rows = pl.ds(pl.multiple_of(b * 128, 128), 128)
            product = ins[K, :, cols].astype(F32) * ins[V, :, cols].astype(F32)
            gate = ins[G, :, cols].astype(F32) * ins[Q, :, cols].astype(F32)
            packed.reshape(GROUPS, 3, width, 128)[g, 0, rows, :] = product.astype(BF).T
            packed.reshape(GROUPS, 3, width, 128)[g, 1, rows, :] = gate.astype(BF).T
            packed.reshape(GROUPS, 3, width, 128)[g, 2, rows, :] = ins[H, :, cols].T
            return carry

        lax.fori_loop(0, width // 128, block, 0)

    def send_in(g, first=False):
        def to(o, i):
            pltpu.make_async_remote_copy(
                src_ref=packed.at[g, :, pl.ds((o * 16 + i) * pairs, pairs)],
                dst_ref=held.at[g, :, :, pl.ds(me * 2, 2), :],
                send_sem=in_send,
                recv_sem=in_recv.at[g],
                device_id=(o, i),
                device_id_type=MESH,
            ).start()

        def one(k, carry):
            to(*target(k))
            return carry

        pltpu.make_async_copy(
            packed.at[g, :, pl.ds(me * pairs, pairs)],
            held.at[g, :, :, pl.ds(me * 2, 2), :],
            in_recv.at[g],
        ).start()
        if first:
            entered(0, near_count)
            for offset in sorted(offsets, key=lambda f: -hops(f)):
                if hops(offset) <= REACH:
                    to(*at_offset(*offset))
            entered(1, far_count)
            for offset in sorted(offsets, key=hops):
                if hops(offset) > REACH:
                    to(*at_offset(*offset))
        else:
            lax.fori_loop(1, DEVICES, one, 0)

    def send_out(g, place, far_first=False):
        def to(o, i):
            pltpu.make_async_remote_copy(
                src_ref=made.at[g, :, :, pl.ds((o * 16 + i) * 2, 2), :],
                dst_ref=place.at[:, pl.ds(me * pairs, pairs)],
                send_sem=out_send,
                recv_sem=out_recv.at[g],
                device_id=(o, i),
                device_id_type=MESH,
            ).start()

        def one(k, carry):
            to(*target(k))
            return carry

        pltpu.make_async_copy(
            made.at[g, :, :, pl.ds(me * 2, 2), :],
            place.at[:, pl.ds(me * pairs, pairs)],
            out_recv.at[g],
        ).start()
        if far_first:
            for offset in sorted(offsets, key=lambda f: hops(f) <= 2):
                to(*at_offset(*offset))
        else:
            lax.fori_loop(1, DEVICES, one, 0)

    def transform(g, h):
        wr, wi = tw_ref[0], tw_ref[1]
        pair = h * 2
        for n in range(3):
            rhs = jnp.concatenate([held[g, n, pair], held[g, n, pair + 1]], axis=1)
            one = jnp.dot(t1_ref[...], rhs, preferred_element_type=F32)
            for e in range(2):
                for p in range(2):
                    re = one[e * 256 : e * 256 + 128, p * 128 : p * 128 + 128]
                    im = one[e * 256 + 128 : e * 256 + 256, p * 128 : p * 128 + 128]
                    ch = p * 2 + e
                    part[n, ch, :, 0:128] = (re * wr + im * wi).astype(BF)
                    part[n, ch, :, 128:256] = (im * wr - re * wi).astype(BF)
        for ch in range(4):
            sp = []
            for n in range(3):
                sp.append(jnp.dot(part[n, ch], t2_ref[...], preferred_element_type=F32))
            vr, vi = sp[0][:, :128], sp[0][:, 128:]
            gr, gi = sp[1][:, :128], sp[1][:, 128:]
            fr, fi = sp[2][:, :128], sp[2][:, 128:]
            prods = (
                (vr * fr - vi * fi, vr * fi + vi * fr),
                (fr * gr + fi * gi, fr * gi - fi * gr),
                (vr * gr + vi * gi, vr * gi - vi * gr),
            )
            for n in range(3):
                qq = jnp.concatenate([prods[n][0].astype(BF), prods[n][1].astype(BF)], axis=1)
                three = jnp.dot(qq, t3_ref[...], preferred_element_type=F32)
                re, im = three[:, :128], three[:, 128:]
                p, e = ch // 2, ch % 2
                spec[n, e * 256 : e * 256 + 128, p * 128 : p * 128 + 128] = (
                    re * wr - im * wi
                ).astype(BF)
                spec[n, e * 256 + 128 : e * 256 + 256, p * 128 : p * 128 + 128] = (
                    im * wr + re * wi
                ).astype(BF)
        for n in range(3):
            four = jnp.dot(t4_ref[...], spec[n], preferred_element_type=F32)
            if n == 2:
                four = four * (1.0 / 128.0)
            for p in range(2):
                made[g, n, pair + p] = four[:, p * 128 : p * 128 + 128].astype(BF)

    lane = lax.broadcasted_iota(jnp.int32, (1, 128), 1)
    sub = lax.broadcasted_iota(jnp.int32, (8, 128), 0)

    def direct_sums(g):
        row = jnp.zeros((1, 128), F32)
        for p in range(pairs):
            terms = held[g, 0, p].astype(F32) * held[g, 1, p].astype(F32)
            folded = jnp.sum(terms.reshape(32, 8, 128), axis=0)
            for e in range(2):
                own = jnp.where(lax.rem(sub, 2) == e, folded, 0.0)
                total = jnp.sum(jnp.sum(own, axis=1, keepdims=True), axis=0, keepdims=True)
                row = row + jnp.where(lane == g * per + p * 2 + e, total, 0.0)
        sk_own[...] = sk_own[...] + row

    def send_sums():
        own = sk_own[...]
        sk_own[...] = jnp.where(my_c == 0, own, pltpu.roll(own, per * GROUPS, 1))
        pltpu.make_async_remote_copy(
            src_ref=sk_own,
            dst_ref=sk_near,
            send_sem=near_send,
            recv_sem=near_recv,
            device_id=partner,
            device_id_type=MESH,
        ).start()
        pltpu.make_async_copy(sk_near, sk_near, near_recv).wait()
        sk_row[...] = sk_own[...] + sk_near[...]

    def pass_sums():
        chip = pl.ds(lax.div(me, 2), 1)
        pltpu.make_async_copy(sk_row, sk_all.at[chip, :], sk_recv).start()
        for offset in sorted(offsets, key=lambda f: hops(f) <= 2):
            if offset[0] == 0:
                pltpu.make_async_remote_copy(
                    src_ref=sk_row,
                    dst_ref=sk_all.at[chip, :],
                    send_sem=sk_send,
                    recv_sem=sk_recv,
                    device_id=at_offset(*offset),
                    device_id_type=MESH,
                ).start()

    def spread_sums():
        pltpu.make_async_copy(sk_all, sk_all, sk_recv).wait()
        rows = lax.broadcasted_iota(jnp.int32, (64, 128), 0)
        cols = lax.broadcasted_iota(jnp.int32, (64, 128), 1)
        mine = lax.div(cols, 16) == lax.rem(rows, 8)
        source = lax.broadcasted_iota(jnp.int32, (128, 128), 0)
        place = lax.broadcasted_iota(jnp.int32, (128, 128), 1)
        base = lax.rem(lax.div(place, per), 2) * (per * GROUPS) + lax.rem(place, per)
        for g in range(GROUPS):
            pick = (source == base + g * per).astype(F32)
            wide = jnp.dot(
                sk_all[...], pick, preferred_element_type=F32, precision=lax.Precision.HIGHEST
            )
            kept = jnp.where(mine, wide, 0.0)
            sk_ref[g * 8 : g * 8 + 8, :] = jnp.sum(kept.reshape(8, 8, 128), axis=1) * (
                1.0 / 128.0
            )

    outs = (lo_ref, qg_ref, kg_ref, vg_ref, fg_ref)

    def finish(g):
        pltpu.make_async_copy(back.at[g], back.at[g], out_recv.at[g]).wait()

        def block(b, carry):
            cols = block_cols(g, b)
            rows = pl.ds(pl.multiple_of(b * 128, 128), 128)
            views = back.reshape(GROUPS - 1, 3, width, 128)
            results = results_of(
                [views[g, n, rows, :] for n in range(3)],
                [ins[n, :, cols] for n in range(4)],
                gain_ref[pl.ds(g * (width // 128) + b, 1), :],
            )
            for n in range(5):
                outs[n][:, cols] = results[n]
            return carry

        lax.fori_loop(0, width // 128, block, 0)

    sk_own[...] = jnp.zeros_like(sk_own)
    prepare(0)
    send_in(0, first=True)

    def ahead(g, carry):
        prepare(g)
        send_in(g)
        return carry

    lax.fori_loop(1, GROUPS, ahead, 0)

    for n, (source, place) in enumerate(fixed):
        pltpu.make_async_copy(source, place, table_sem.at[n]).wait()

    def middle(g, carry):
        pltpu.make_async_copy(held.at[g], held.at[g], in_recv.at[g]).wait()

        def half(h, inside):
            transform(g, h)
            return inside

        direct_sums(g)

        @pl.when(g == GROUPS - 1)
        def _():
            send_sums()

        lax.fori_loop(0, pairs // 2, half, 0)

        @pl.when(g == GROUPS - 1)
        def _():
            pass_sums()

        @pl.when(g < GROUPS - 1)
        def _():
            send_out(g, back.at[g])

        @pl.when(g == GROUPS - 1)
        def _():
            send_out(g, final, far_first=True)

        return carry

    lax.fori_loop(0, GROUPS, middle, 0)

    def ending(g, carry):
        finish(g)
        return carry

    lax.fori_loop(0, GROUPS - 1, ending, 0)
    spread_sums()
    everyone = held.at[:, :, :, pl.ds(0, 2 * (DEVICES - 1)), :]
    pltpu.make_async_copy(everyone, everyone, in_send).wait()
    pltpu.make_async_copy(sk_near, sk_near, near_send).wait()
    sums = sk_all.at[pl.ds(0, DEVICES // 2 - 1), :]
    pltpu.make_async_copy(sums, sums, sk_send).wait()
    pltpu.make_async_copy(final, final, out_recv.at[GROUPS - 1]).wait()
    pltpu.make_async_copy(everyone, everyone, out_send).wait()


def results_of(sums, rows, gain):
    conv, corr = sums[0].T.astype(F32), sums[1].T.astype(F32)
    kk, vv, gg, qq = (r.astype(F32) for r in rows)
    product = (kk * vv).astype(BF).astype(F32)
    mixing = conv + gain * product
    carried = corr + gain * (gg * qq)
    return (
        (qq * mixing).astype(BF),
        (gg * mixing).astype(BF),
        (carried * vv).astype(BF),
        (carried * kk).astype(BF),
        sums[2].T,
    )


def deliver(*refs):
    early, (ins, final, gain_ref, sums) = refs[:5], refs[5:9]
    whole, sums_out = refs[9:14], refs[14]
    late, sem = refs[15], refs[16]
    channels = whole[0].shape[1]
    width = channels // GROUPS
    first = channels - width
    parts = 2
    step = width // parts
    copies = [
        pltpu.make_async_copy(early[n], whole[n].at[:, pl.ds(0, first)], sem.at[n])
        for n in range(5)
    ]
    copies.append(pltpu.make_async_copy(sums, sums_out, sem.at[5]))
    for copy in copies:
        copy.start()
    views = final.reshape(3, width, 128)
    for part in range(parts):

        def block(b, carry):
            at = pl.multiple_of(part * step + b * 128, 128)
            cols = pl.ds(first + at, 128)
            results = results_of(
                [views[n, pl.ds(at, 128), :] for n in range(3)],
                [ins[n, :, cols] for n in range(4)],
                gain_ref[pl.ds((first + part * step) // 128 + b, 1), :],
            )
            for n in range(5):
                late[n, :, pl.ds(at, 128)] = results[n]
            return carry

        lax.fori_loop(0, step // 128, block, 0)
        for n in range(5):
            copies.append(
                pltpu.make_async_copy(
                    late.at[n, :, pl.ds(part * step, step)],
                    whole[n].at[:, pl.ds(first + part * step, step)],
                    sem.at[6 + part * 5 + n],
                )
            )
            copies[-1].start()
    for copy in copies:
        copy.wait()


def body(query_rows, key_rows, value_rows, out_grad, filter_rows, skip_gain):
    tokens, channels = query_rows.shape
    length = tokens * DEVICES
    width = channels // GROUPS
    per = width // DEVICES
    tables = [jnp.asarray(t) for t in coefficient_tables(tokens, DEVICES, length)]
    rows = jax.ShapeDtypeStruct((tokens, channels), BF)
    anywhere = pl.BlockSpec(memory_space=pl.ANY)
    dma = pltpu.SemaphoreType.DMA
    sums = jax.ShapeDtypeStruct((channels // 128, 128), F32)
    early = jax.ShapeDtypeStruct((tokens, channels - width), BF)
    hbm = pl.BlockSpec(memory_space=pltpu.HBM)
    vmem = pl.BlockSpec(memory_space=pltpu.VMEM)
    handed = pl.pallas_call(
        kernel,
        out_shape=[early] * 5
        + [
            jax.ShapeDtypeStruct((5, tokens, channels), BF),
            jax.ShapeDtypeStruct((3, width // 2, 2, 128), BF),
            sums,
            sums,
        ],
        in_specs=[hbm] * 11,
        out_specs=[vmem] * 9,
        scratch_shapes=[
            *[pltpu.VMEM(t.shape, t.dtype) for t in tables],
            pltpu.VMEM((GROUPS, 3, width // 2, 2, 128), BF),
            pltpu.VMEM((GROUPS, 3, per // 2, 2 * DEVICES, 128), BF),
            pltpu.VMEM((GROUPS, 3, per // 2, 2 * DEVICES, 128), BF),
            pltpu.VMEM((GROUPS - 1, 3, width // 2, 2, 128), BF),
            pltpu.VMEM((3, 4, DEVICES, 256), BF),
            pltpu.VMEM((3, 4 * DEVICES, 256), BF),
            pltpu.VMEM((1, 128), F32),
            pltpu.VMEM((1, 128), F32),
            pltpu.VMEM((1, 128), F32),
            pltpu.VMEM((DEVICES // 2, 128), F32),
            dma((5, GROUPS)),
            dma((6,)),
            dma,
            dma((GROUPS,)),
            dma,
            dma((GROUPS,)),
            dma,
            dma,
            dma,
            dma,
            pltpu.SemaphoreType.REGULAR,
        ],
        compiler_params=pltpu.CompilerParams(
            collective_id=0, has_side_effects=True, vmem_limit_bytes=VMEM_MAIN * 1024 * 1024
        ),
        name="hyena",
    )(
        *(
            pltpu.with_memory_space_constraint(a, pltpu.HBM)
            for a in (
                query_rows,
                key_rows,
                value_rows,
                out_grad,
                filter_rows,
                skip_gain.reshape(channels // 128, 128),
                *tables,
            )
        )
    )
    results = pl.pallas_call(
        deliver,
        out_shape=[rows] * 5 + [sums],
        in_specs=[anywhere] * 5 + [vmem] * 3 + [anywhere],
        out_specs=[hbm] * 6,
        scratch_shapes=[pltpu.VMEM((5, tokens, width), BF), dma((16,))],
        compiler_params=pltpu.CompilerParams(vmem_limit_bytes=VMEM_LAST * 1024 * 1024),
        name="deliver",
    )(*handed)
    return (*results[:5], results[5].reshape(channels))


def solution(mesh):
    rows = P(("outer", "inner"), None)
    return jax.shard_map(
        body,
        mesh=mesh,
        in_specs=(rows, rows, rows, rows, rows, P()),
        out_specs=(rows, rows, rows, rows, rows, P()),
        check_vma=False,
    )
```
